128 devices in a mesh: seq: 16 (over x, y), tp: 8 (over z, core).
Axes of the slice: x: 4, y: 4, z: 4, core: 2. Of those that a mesh axis runs over, the one named last changes fastest.
Arguments:
- patches: bfloat16 [8192, 1280], P('seq'), may hold values from -6 to 6
- image_ids: int32 [2048], replicated, may hold values from 0 to 31, never falling along the last dimension, each value on 1 to 128 neighbouring positions
- vision_gain: float32 [1280], replicated, may hold values from 0.5 to 2
- v_query: bfloat16 [1280, 1280], P(None, 'tp'), may hold values from -0.15625 to 0.15625
- v_key: bfloat16 [1280, 1280], P(None, 'tp'), may hold values from -0.15625 to 0.15625
- v_value: bfloat16 [1280, 1280], P(None, 'tp'), may hold values from -0.15625 to 0.15625
- v_out: bfloat16 [1280, 1280], P('tp'), may hold values from -0.625 to 0.625
- merge_gain: float32 [1280], replicated, may hold values from 0.5 to 1.5
- merge_up: bfloat16 [5120, 5120], P('seq', 'tp'), may hold values from -0.078125 to 0.078125
- merge_down: bfloat16 [5120, 8192], P('tp', 'seq'), may hold values from -0.078125 to 0.078125
- owners: int32 [2048, 1], replicated, may hold values from 0 to 15; in each aligned block of 128 rows (0 to 127, 128 to 255, ...) at most 16 rows name the same one
- text_embed: bfloat16 [4096, 8192], P('seq', 'tp'), may hold values from -6 to 6
- segment_ids: int32 [4096], P('seq'), may hold values from 0 to 63, never falling along the last dimension, each value on 1 to 256 neighbouring positions
- lang_gain: float32 [8192], replicated, may hold values from 0.5 to 2
- l_query: bfloat16 [8192, 4096], P(None, 'tp'), may hold values from -0.0625 to 0.0625
- l_key: bfloat16 [8192, 1024], P(None, 'tp'), may hold values from -0.0625 to 0.0625
- l_value: bfloat16 [8192, 1024], P(None, 'tp'), may hold values from -0.0625 to 0.0625
- l_out: bfloat16 [4096, 8192], P('tp'), may hold values from -0.09375 to 0.09375
Outputs:
- layer_out: bfloat16 [4096, 8192], P('seq', 'tp')
The draws below stay inside these ranges and needn't reach their ends.
Inputs may be any that keep to these rules, and one draw needn't show every extreme that they name: `image_ids`: never falling; each image spans 1 to 128 merged tokens, one exactly 128. `owners`: among the rows of one device (aligned blocks of 128 rows) at most 16 name the same packed sequence. `segment_ids`: never falling; each document holds 1 to 256 slots, one exactly 256.
All inputs are finite; a program needn't handle non-finite values.
Results may differ from the reference program's by a relative error of at most 0.019.
Values may be sent and summed in bfloat16 or wider, within the bound.
No kernel may reach another device: no remote copies, remote signals or barrier semaphores. Data moves between devices by JAX's collectives and lax.ppermute only.
A program may use at most 128 MiB of HBM per device.

```python
import math
import jax
import jax.numpy as jnp
import numpy as np
from jax import lax

DV = 1280
VHEADS = 16
MHID = 5120
D = 8192
LHEADS = 32
LKV = 8
LHD = 128
PAT_DEV = 512
MIN = 5120
QW = 4096
KW = 1024
MERGED_DEV = 128
CAP = 256
PAIR_CAP = 16
PATCHES = 8192
MERGED = 2048
SLOTS = 4096
IMAGES = 32
SEGS = 64
N_SEQ = 16
N_TP = 8


def gain_draw(key, width):
    return jax.random.uniform(key, (width,), jnp.float32, 0.6, 1.4)


def draw_vision_gain(key, part):
    return gain_draw(jax.random.fold_in(key, 11), DV)


def draw_lang_gain(key, part):
    return gain_draw(jax.random.fold_in(key, 23), D)


def steps_of(rng, dims, pieces, least, top_value):
    gain, own = 1.0, jax.random.fold_in(rng, 6)
    for axis_at, shards_of in pieces:
        steps = jnp.exp(jax.random.uniform(jax.random.fold_in(own, axis_at), (shards_of,), jnp.float32, least / len(pieces), top_value / len(pieces)))
        gain = gain * jnp.repeat(steps, dims[axis_at] // shards_of).reshape([-1 if axis == axis_at else 1 for axis in range(len(dims))])
    return gain


def split_up(amount, total, reach, slope):
    weights = [(1 << 20) // math.isqrt(rank ** slope) + 1 for rank in range(2, amount + 1)]
    rest, holding = total - reach - (amount - 1), [1] * (amount - 1)
    while rest > 0:
        movable = [i for i in range(amount - 1) if holding[i] < reach]
        pool, remaining = sum([weights[i] for i in movable]), rest
        for i in movable:
            addition = min(reach - holding[i], max(1, remaining * weights[i] // pool), rest)
            holding[i] = holding[i] + addition
            rest = rest - addition
    return np.array([reach] + holding)


def uneven(stream_key, number_of, total, bound, lean):
    if number_of == 2:
        one = jax.random.randint(stream_key, (), max(1, total - bound), min(bound, total - 1) + 1)
        return jnp.stack([one, total - one])
    tallies = jnp.asarray(split_up(number_of, total, bound, lean), jnp.int32)
    couples = (number_of - 1) // 2
    donor, sink = tallies[1:1 + 2 * couples:2], tallies[2:2 + 2 * couples:2]
    margin = jnp.minimum(donor - 1, bound - sink)
    shifted = jax.random.randint(jax.random.fold_in(stream_key, 1), (couples,), 0, 1 << 20) % (margin + 1)
    tallies = tallies.at[1:1 + 2 * couples:2].set(donor - shifted).at[2:2 + 2 * couples:2].set(sink + shifted)
    return tallies[jax.random.permutation(jax.random.fold_in(stream_key, 2), number_of)]


def routed_block(own_key, own, number, rows, number_of, top, reach, slope):
    ranking = jax.random.permutation(own_key, number_of)
    crowded, common = portions_of(number_of, rows * top, reach, slope, True), portions_of(number_of, rows * top, reach, slope, False)
    places = jnp.arange(number_of)

    def named(sizes, turn):
        used = int((sizes > 0).sum())
        fixed = max(1, used // 4)
        passed = fixed + (places - fixed + turn * (used - fixed)) % max(1, number_of - fixed)
        return jnp.zeros((number_of,), jnp.int32).at[ranking[jnp.where(places < fixed, places, passed)]].set(jnp.asarray(sizes, jnp.int32))

    sizes = jnp.where(number % 4 == 0, named(crowded, number // 4), named(common, number - number // 4 - 1))
    mixed = jax.random.permutation(jax.random.fold_in(own, 3), number_of)
    donor, sink = mixed[0:number_of // 2 * 2:2], mixed[1:number_of // 2 * 2:2]
    slack = jnp.minimum(sizes[donor] - 1, reach - sizes[sink]) // 2
    slack = jnp.where((donor == ranking[0]) | (sink == ranking[0]) | (sizes[sink] == 0), 0, jnp.maximum(slack, 0))
    passed = jax.random.randint(jax.random.fold_in(own, 4), (number_of // 2,), 0, 1 << 20) % (slack + 1)
    sizes = sizes.at[donor].add(-passed).at[sink].add(passed)
    labels = jnp.searchsorted(jnp.cumsum(sizes), jnp.arange(rows * top), side="right").astype(jnp.int32)
    grid = labels.reshape(top, rows).T
    grid = grid[jax.random.permutation(jax.random.fold_in(own, 1), rows)]
    turn = jax.random.randint(jax.random.fold_in(own, 2), (rows, 1), 0, top)
    return jnp.take_along_axis(grid, (jnp.arange(top)[None, :] + turn) % top, axis=1)


def portions_of(amount, total, limit, lean, full):
    portions = [(1 << 20) // math.isqrt(grade ** lean) + 1 for grade in range(1, amount + 1)]
    largest = limit if full else min(limit, max(-(-total // amount), total * portions[0] // sum(portions)))
    least = 1 if total - largest >= amount - 1 else 0
    given, surplus = [largest] + [least] * (amount - 1), total - largest - least * (amount - 1)
    while surplus > 0:
        movable = [i for i in range(1, amount) if given[i] < largest] or [i for i in range(1, amount) if given[i] < limit]
        pool, budget = sum([portions[i] for i in movable]), surplus
        for i in movable:
            extra = min(limit - given[i], max(1, budget * portions[i] // pool), surplus)
            given[i] = given[i] + extra
            surplus = surplus - extra
    return np.array(given)


def noise(key, dims, deviation, reach, pieces=(), kind=jnp.bfloat16):
    values = jax.random.normal(key, dims, jnp.float32) * deviation
    if len(pieces) > 0:
        values = steps_of(key, dims, pieces, -0.22, 0.18) * values
    return jnp.clip(values, min=-reach, max=reach).astype(kind)


def setup_inputs(seed: int = 0) -> dict:
    key_of = jax.random.split(jax.random.key(seed), 19)
    patches = noise(key_of[0], (PATCHES, DV), 1.0, 6.0, ((0, 16),))
    image_ids = jnp.searchsorted(jnp.cumsum(uneven(key_of[1], IMAGES, MERGED, MERGED_DEV, 2)), jnp.arange(MERGED), side="right").astype(jnp.int32)
    vision_gain = draw_vision_gain(jax.random.fold_in(key_of[18], 71), 0)
    v_query = noise(key_of[3], (DV, DV), DV ** -0.5, 0.15625, ((1, 8),))
    v_key = noise(key_of[4], (DV, DV), DV ** -0.5, 0.15625, ((1, 8),))
    v_value = noise(key_of[5], (DV, DV), DV ** -0.5, 0.15625, ((1, 8),))
    v_out = noise(key_of[6], (DV, DV), (DV // 16) ** -0.5, 0.625, ((0, 8),))
    merge_gain = jnp.clip(1.0 + 0.1 * jax.random.normal(key_of[7], (DV,), jnp.float32), 0.5, 1.5)
    merge_up = noise(key_of[8], (MIN, MHID), MIN ** -0.5, 0.078125, ((0, 16), (1, 8)))
    merge_down = noise(key_of[9], (MHID, D), MHID ** -0.5, 0.078125, ((0, 8), (1, 16)))
    owners_keys = jax.random.split(jax.random.fold_in(key_of[10], 1), MERGED // MERGED_DEV)
    owners_turns = jax.random.permutation(jax.random.fold_in(key_of[10], 3), MERGED // MERGED_DEV)
    owners = jax.vmap(lambda own, number: routed_block(jax.random.fold_in(key_of[10], 2), own, number, MERGED_DEV, N_SEQ, 1, PAIR_CAP, 2))(owners_keys, owners_turns).reshape((MERGED, 1))
    text_embed = noise(key_of[11], (SLOTS, D), 1.0, 6.0, ((0, 16), (1, 8)))
    segment_ids = jnp.searchsorted(jnp.cumsum(uneven(key_of[12], SEGS, SLOTS, CAP, 2)), jnp.arange(SLOTS), side="right").astype(jnp.int32)
    lang_gain = draw_lang_gain(jax.random.fold_in(key_of[18], 71), 0)
    l_query = noise(key_of[14], (D, QW), D ** -0.5, 0.0625, ((1, 8),))
    l_key = noise(key_of[15], (D, KW), D ** -0.5, 0.0625, ((1, 8),))
    l_value = noise(key_of[16], (D, KW), D ** -0.5, 0.0625, ((1, 8),))
    l_out = noise(key_of[17], (QW, D), QW ** -0.5, 0.09375, ((0, 8),))
    return {"patches": patches, "image_ids": image_ids, "vision_gain": vision_gain, "v_query": v_query, "v_key": v_key, "v_value": v_value, "v_out": v_out, "merge_gain": merge_gain, "merge_up": merge_up, "merge_down": merge_down, "owners": owners, "text_embed": text_embed, "segment_ids": segment_ids, "lang_gain": lang_gain, "l_query": l_query, "l_key": l_key, "l_value": l_value, "l_out": l_out}


EPSILON = 1e-06
NEG_FILL = -1e+30

def rms_scaled(values, norm_gain):
    mean_square = lax.optimization_barrier(jnp.mean(values * values, axis=-1, keepdims=True))
    return (values * lax.rsqrt(mean_square + EPSILON) * norm_gain).astype(jnp.bfloat16)

def narrowed(values):
    return lax.optimization_barrier(values.astype(jnp.bfloat16)).astype(jnp.float32)

def block_sum(left, right):
    width = left.shape[1] // N_TP
    totals = jnp.zeros((left.shape[0], right.shape[1]), jnp.float32)
    for block_index in range(N_TP):
        lower = block_index * width
        partial_value = jnp.dot(left[:, lower:lower + width], right[lower:lower + width], preferred_element_type=jnp.float32)
        totals = totals + narrowed(partial_value)
    return totals

def masked_mix(query_rows, key_rows, value_rows, allowed, score_scale):
    scores = jnp.einsum('qhd,nhd->hqn', query_rows, key_rows) * score_scale
    scores = jnp.where(allowed[None], scores, NEG_FILL)
    highest = lax.optimization_barrier(jnp.max(scores, axis=-1, keepdims=True))
    weights_raw = jnp.where(allowed[None], jnp.exp(scores - highest), 0.0)
    totals = lax.optimization_barrier(jnp.sum(weights_raw, axis=-1))
    mixed = jnp.einsum('hqn,nhd->qhd', narrowed(weights_raw), value_rows)
    return mixed / jnp.transpose(totals)[:, :, None]

def vision_attention(query_rows, key_rows, value_rows, patch_ids):
    head_size = DV // VHEADS
    score_scale = 1.0 / math.sqrt(head_size)
    padded_keys = jnp.pad(key_rows, ((PAT_DEV, PAT_DEV), (0, 0), (0, 0)))
    padded_values = jnp.pad(value_rows, ((PAT_DEV, PAT_DEV), (0, 0), (0, 0)))
    padded_ids = jnp.pad(patch_ids, (PAT_DEV, PAT_DEV), constant_values=-1)

    def one_block(block_index):
        first_row = (block_index * PAT_DEV).astype(jnp.int32)
        block_queries = lax.dynamic_slice_in_dim(query_rows, first_row, PAT_DEV, 0).astype(jnp.float32)
        block_keys = lax.dynamic_slice_in_dim(padded_keys, first_row, 3 * PAT_DEV, 0).astype(jnp.float32)
        block_values = lax.dynamic_slice_in_dim(padded_values, first_row, 3 * PAT_DEV, 0).astype(jnp.float32)
        query_ids = lax.dynamic_slice_in_dim(patch_ids, first_row, PAT_DEV, 0)
        key_ids = lax.dynamic_slice_in_dim(padded_ids, first_row, 3 * PAT_DEV, 0)
        allowed = query_ids[:, None] == key_ids[None, :]
        mixed = masked_mix(block_queries, block_keys, block_values, allowed, score_scale)
        return mixed.astype(jnp.bfloat16)
    blocks = lax.map(one_block, jnp.arange(N_SEQ, dtype=jnp.int32))
    return blocks.reshape(PATCHES, DV)

def language_attention(query_rows, key_rows, value_rows, segment_ids):
    group_size = LHEADS // LKV
    query_grid = query_rows.astype(jnp.float32).reshape(N_SEQ, CAP, LKV, group_size, LHD)
    key_grid = key_rows.astype(jnp.float32).reshape(N_SEQ, CAP, LKV, LHD)
    value_grid = value_rows.astype(jnp.float32).reshape(N_SEQ, CAP, LKV, LHD)
    segment_grid = segment_ids.reshape(N_SEQ, CAP)
    position = jnp.arange(CAP, dtype=jnp.int32)
    allowed = (segment_grid[:, :, None] == segment_grid[:, None, :]) & (position[None, None, :] <= position[None, :, None])
    scores = jnp.einsum('bqkgd,bnkd->bkgqn', query_grid, key_grid) / math.sqrt(LHD)
    scores = jnp.where(allowed[:, None, None], scores, NEG_FILL)
    highest = lax.optimization_barrier(jnp.max(scores, axis=-1, keepdims=True))
    weights_raw = jnp.where(allowed[:, None, None], jnp.exp(scores - highest), 0.0)
    totals = lax.optimization_barrier(jnp.sum(weights_raw, axis=-1))
    mixed = jnp.einsum('bkgqn,bnkd->bqkgd', narrowed(weights_raw), value_grid)
    mixed = mixed / jnp.transpose(totals, (0, 3, 1, 2))[..., None]
    return mixed.reshape(SLOTS, LHEADS * LHD).astype(jnp.bfloat16)

def reference(patches, image_ids, vision_gain, v_query, v_key, v_value, v_out, merge_gain, merge_up, merge_down, owners, text_embed, segment_ids, lang_gain, l_query, l_key, l_value, l_out):
    head_size = DV // VHEADS
    patch_ids = jnp.repeat(image_ids, 4)
    vision_state = patches.astype(jnp.float32)
    normed = rms_scaled(vision_state, vision_gain)
    query_rows = jnp.dot(normed, v_query, preferred_element_type=jnp.float32).astype(jnp.bfloat16).reshape(PATCHES, VHEADS, head_size)
    key_rows = jnp.dot(normed, v_key, preferred_element_type=jnp.float32).astype(jnp.bfloat16).reshape(PATCHES, VHEADS, head_size)
    value_rows = jnp.dot(normed, v_value, preferred_element_type=jnp.float32).astype(jnp.bfloat16).reshape(PATCHES, VHEADS, head_size)
    attended = vision_attention(query_rows, key_rows, value_rows, patch_ids)
    vision_state = vision_state + block_sum(attended, v_out)
    merge_input = rms_scaled(vision_state, merge_gain).reshape(MERGED, 4 * DV)
    hidden = jax.nn.gelu(jnp.dot(merge_input, merge_up, preferred_element_type=jnp.float32), approximate=False).astype(jnp.bfloat16)
    merged = block_sum(hidden, merge_down).astype(jnp.bfloat16)
    destination = owners[:, 0].astype(jnp.int32)
    one_hot = (destination[:, None] == jnp.arange(N_SEQ, dtype=jnp.int32)[None, :]).astype(jnp.int32)
    earlier = lax.optimization_barrier(jnp.sum((jnp.cumsum(one_hot, axis=0) - one_hot) * one_hot, axis=1))
    slot_index = (destination * CAP + earlier).astype(jnp.int32)
    filled = text_embed.at[slot_index].set(merged)
    lang_normed = rms_scaled(filled.astype(jnp.float32), lang_gain)
    lang_query = jnp.dot(lang_normed, l_query, preferred_element_type=jnp.float32).astype(jnp.bfloat16)
    lang_key = jnp.dot(lang_normed, l_key, preferred_element_type=jnp.float32).astype(jnp.bfloat16)
    lang_value = jnp.dot(lang_normed, l_value, preferred_element_type=jnp.float32).astype(jnp.bfloat16)
    lang_attended = language_attention(lang_query, lang_key, lang_value, segment_ids)
    return (filled.astype(jnp.float32) + block_sum(lang_attended, l_out)).astype(jnp.bfloat16)
```

```python
import math

import jax
import jax.numpy as jnp
from jax import lax
from jax.experimental import pallas as pl
from jax.experimental.pallas import tpu as pltpu
from jax.sharding import Mesh
from jax.sharding import PartitionSpec as P

DV = 1280
VHEADS = 16
D = 8192
LHD = 128
HEAD = DV // VHEADS
EPSILON = 1e-06
NEG_FILL = -1e30
BF = jnp.bfloat16
F32 = jnp.float32


def shift(value, axis, step):
    count = lax.axis_size(axis)
    return lax.ppermute(value, axis, [(i, (i + step) % count) for i in range(count)])


def after(value, other):
    return lax.optimization_barrier((value, other))[0]


def gather_ring(value, axis):
    half = value.shape[0] // 2
    before = shift(value, axis, 1)
    behind = shift(value, axis, -1)
    low = shift(before[:half], axis, 1)
    high = shift(behind[half:], axis, -1)
    return [value, before, jnp.concatenate([low, high], axis=0), behind]


def gather_tp(value):
    blocks = []
    for block in gather_ring(value, "z"):
        blocks += [block, shift(block, "c", 1)]
    return blocks


def reduce_ring(blocks, axis, from_before=lambda v: v, from_after=lambda v: v):
    half = blocks[2].shape[0] // 2
    up = from_before(shift(blocks[2][:half].astype(BF), axis, 1))
    down = from_after(shift(blocks[2][half:].astype(BF), axis, -1))
    nxt = jnp.concatenate([blocks[1][:half].astype(F32) + up.astype(F32), blocks[1][half:].astype(F32)], axis=0)
    prv = jnp.concatenate([blocks[3][:half].astype(F32), blocks[3][half:].astype(F32) + down.astype(F32)], axis=0)
    got = from_before(shift(nxt.astype(BF), axis, 1))
    got2 = from_after(shift(prv.astype(BF), axis, -1))
    return blocks[0].astype(F32) + got.astype(F32) + got2.astype(F32)


def in_place(blocks, starts, count):
    out = jnp.zeros((count, *blocks[0].shape), blocks[0].dtype)
    for block, start in zip(blocks, starts):
        out = lax.dynamic_update_index_in_dim(out, block, start, 0)
    return out


def rms_scaled(values, norm_gain):
    mean_square = jnp.mean(values * values, axis=-1, keepdims=True)
    return (values * lax.rsqrt(mean_square + EPSILON) * norm_gain).astype(BF)


def vision_kernel(x_ref, q_ref, k0, k1, k2, v0, v1, v2, qid_ref, kid_ref, out_ref):
    rows, count = q_ref.shape
    tokens = count // 4
    column = lax.broadcasted_iota(jnp.int32, (count, count), 1)
    source = lax.broadcasted_iota(jnp.int32, (count, count), 0)
    wanted = 4 * (column % tokens) + (column // tokens + x_ref[0]) % 4
    order = (source == wanted).astype(F32).astype(BF)
    queries = jnp.dot(q_ref[...], order, preferred_element_type=F32).astype(BF)
    keys = jnp.concatenate([k0[...], k1[...], k2[...]], axis=1)
    values = jnp.concatenate([v0[...], v1[...], v2[...]], axis=1)
    wide = count // 2
    allowed = kid_ref[...] == qid_ref[:, :wide]
    scale = 1.0 / math.sqrt(HEAD)
    for part in range(2):
        for head in range(rows // HEAD):
            lower = head * HEAD
            scores = lax.dot_general(
                keys[lower : lower + HEAD],
                queries[lower : lower + HEAD, part * wide : (part + 1) * wide],
                (((0,), (0,)), ((), ())),
                preferred_element_type=F32,
            )
            scores = jnp.where(allowed, scores * scale, NEG_FILL)
            highest = jnp.max(scores, axis=0, keepdims=True)
            weights = jnp.where(allowed, jnp.exp(scores - highest), 0.0)
            totals = jnp.sum(weights, axis=0, keepdims=True)
            mixed = jnp.dot(values[lower : lower + HEAD], weights.astype(BF), preferred_element_type=F32)
            out_ref[lower : lower + HEAD, part * wide : (part + 1) * wide] = (mixed / totals).astype(BF)


def language_kernel(in_ref, text_ref, place_ref, vis_ref, sega_ref, segb_ref, out_ref):
    slots = text_ref.shape[0]
    row = lax.broadcasted_iota(jnp.int32, (slots, slots), 0)
    col = lax.broadcasted_iota(jnp.int32, (slots, slots), 1)
    spread = (row == place_ref[...]).astype(F32).astype(BF)
    placed = jnp.dot(spread, in_ref[...], preferred_element_type=F32)
    qkv = jnp.where(vis_ref[...] > 0, placed, text_ref[...].astype(F32)).astype(BF)
    allowed = (sega_ref[...] == segb_ref[...]) & (col <= row)
    width = out_ref.shape[1]
    keys, values = qkv[:, width : width + LHD], qkv[:, width + LHD :]
    for head in range(width // LHD):
        scores = lax.dot_general(
            qkv[:, head * LHD : (head + 1) * LHD], keys, (((1,), (1,)), ((), ())), preferred_element_type=F32
        ) * (1.0 / math.sqrt(LHD))
        scores = jnp.where(allowed, scores, NEG_FILL)
        highest = jnp.max(scores, axis=-1, keepdims=True)
        weights = jnp.where(allowed, jnp.exp(scores - highest), 0.0)
        totals = jnp.sum(weights, axis=-1, keepdims=True)
        mixed = jnp.dot(weights.astype(BF), values, preferred_element_type=F32)
        out_ref[:, head * LHD : (head + 1) * LHD] = (mixed / totals).astype(BF)


def blocks_kernel(order_ref, left_ref, right_ref, out_ref):
    out_ref[0] = jnp.dot(left_ref[...], right_ref[...], preferred_element_type=F32).astype(BF)


def column_blocks(left, right, order, width):
    count = order.shape[0]
    return pl.pallas_call(
        blocks_kernel,
        grid_spec=pltpu.PrefetchScalarGridSpec(
            num_scalar_prefetch=1,
            grid=(count,),
            in_specs=[
                pl.BlockSpec(left.shape, lambda i, o: (0, 0)),
                pl.BlockSpec((right.shape[0], width), lambda i, o: (0, o[i])),
            ],
            out_specs=pl.BlockSpec((1, left.shape[0], width), lambda i, o: (i, 0, 0)),
        ),
        out_shape=jax.ShapeDtypeStruct((count, left.shape[0], width), BF),
    )(order, left, right)


def body(
    patches, image_ids, vision_gain, v_query, v_key, v_value, v_out, merge_gain, merge_up, merge_down,
    owners, text_embed, segment_ids, lang_gain, l_query, l_key, l_value, l_out,
):
    x, y, z, c = (lax.axis_index(a) for a in ("x", "y", "z", "c"))
    seq_index = 4 * x + y
    row_count = patches.shape[0]
    tokens = row_count // 4
    local = v_query.shape[1]

    normed = rms_scaled(patches.astype(F32), vision_gain)

    def project(weight):
        return lax.dot_general(weight, normed, (((0,), (1,)), ((), ())), preferred_element_type=F32).astype(BF)

    key_own, value_own = project(v_key), project(v_value)
    seq = ("x", "y")
    key_left, key_right = shift(key_own, seq, 1), shift(key_own, seq, -1)
    value_left, value_right = shift(value_own, seq, 1), shift(value_own, seq, -1)
    query_own = project(v_query)
    padded_ids = jnp.pad(image_ids, (tokens, tokens), constant_values=-1)
    near_ids = lax.dynamic_slice_in_dim(padded_ids, seq_index * tokens, 3 * tokens)
    own_ids = near_ids[tokens : 2 * tokens]
    key_ids = jnp.repeat(near_ids, 4)
    left_ids, mid_ids, right_ids = (key_ids[i * row_count : (i + 1) * row_count] for i in range(3))
    attended = pl.pallas_call(
        vision_kernel,
        in_specs=[pl.BlockSpec(memory_space=pltpu.SMEM)] + [pl.BlockSpec(memory_space=pltpu.VMEM)] * 9,
        out_specs=pl.BlockSpec(memory_space=pltpu.VMEM),
        out_shape=jax.ShapeDtypeStruct((local, row_count), BF),
    )(
        x.reshape(1).astype(jnp.int32),
        query_own, key_own, key_left, key_right, value_own, value_left, value_right,
        jnp.tile(own_ids, 4)[None, :],
        jnp.concatenate([mid_ids, left_ids, right_ids])[:, None],
    )

    early = value_right
    token_at = jnp.arange(tokens, dtype=jnp.int32)
    patch_at = jnp.arange(row_count, dtype=jnp.int32)
    own_patches = []
    for d in range(4):
        pick = (patch_at[None, :] == (4 * token_at + (x + d) % 4)[:, None]).astype(BF)
        picked = jnp.dot(pick, patches, preferred_element_type=F32).astype(BF)
        own_patches.append(picked if d == 0 else shift(picked, "x", d))
    residual = jnp.concatenate(own_patches, axis=0)
    out_weight = jnp.concatenate(gather_tp(after(v_out, key_own)), axis=0)
    back = [(y - d) % 4 for d in range(4)]
    up_weight = in_place(gather_ring(after(merge_up, early), "y"), back, 4).reshape(4 * merge_up.shape[0], -1)

    yh, b = y // 2, y % 2
    down_parts = after(merge_down, early).reshape(4, merge_down.shape[0] // 4, -1)
    moved, at = [], []
    for k in range(4):
        pairs = []
        for sx in range(4):
            for sy in range(4):
                for sz in range(4):
                    for sc in range(2):
                        to = (2 * sc + sy % 2 + k) % 4
                        pairs.append((((sx * 4 + sy) * 4 + sz) * 2 + sc, ((to * 4 + sz) * 4 + sx) * 2 + sy // 2))
        part = lax.dynamic_index_in_dim(down_parts, (2 * c + b + k) % 4, 0, keepdims=False)
        moved.append(lax.ppermute(part, ("x", "y", "z", "c"), pairs))
        slot = (x - k) % 4
        at.append(2 * (slot % 2) + (slot // 2 - c) % 2)
    down_own = in_place(moved, at, 4)
    down_blocks = gather_ring(down_own, "y")
    down_weight = jnp.zeros((2, 4, *down_own.shape[0:0], 2, *down_own.shape[1:]), BF)
    for d, block in enumerate(down_blocks):
        down_weight = lax.dynamic_update_slice(
            down_weight, block.reshape(2, 1, 2, *block.shape[1:]), (0, (z - back[d]) % 4, 0, 0, 0)
        )
    down_weight = down_weight.reshape(2, 8 * down_own.shape[1], -1)

    zc_at = []
    for r in range(4):
        for other in range(2):
            zc_at.append(2 * ((z - r) % 4) + (c + other) % 2)

    def language_rows(rows):
        blocks = in_place(gather_tp(rows), zc_at, 8)
        whole = jnp.moveaxis(blocks, 0, 1).reshape(rows.shape[0], -1)
        lang_normed = rms_scaled(whole.astype(F32), lang_gain)
        return jnp.concatenate(
            [jnp.dot(lang_normed, w, preferred_element_type=F32).astype(BF) for w in (l_query, l_key, l_value)], axis=1
        )

    text_qkv = language_rows(after(text_embed, out_weight))

    att_parts = [attended[:, d * tokens : (d + 1) * tokens] for d in range(4)]
    att_rows = jnp.concatenate([att_parts[0]] + [shift(att_parts[d], "x", d) for d in (1, 2, 3)], axis=1)
    att_all = jnp.concatenate(gather_tp(att_rows), axis=0)
    state = residual.astype(F32) + lax.dot_general(
        att_all, out_weight, (((0,), (0,)), ((), ())), preferred_element_type=F32
    )
    merge_rows = rms_scaled(state, merge_gain)
    up_terms = lax.dot_general(up_weight, merge_rows, (((0,), (1,)), ((), ())), preferred_element_type=F32).astype(BF)
    up_parts = up_terms.reshape(4, -1, row_count)
    up_blocks = [lax.dynamic_index_in_dim(up_parts, (x + e) % 4, 0, keepdims=False) for e in range(4)]
    hidden_sum = reduce_ring(
        up_blocks,
        "x",
        lambda v: jnp.concatenate([v[:, 3 * tokens :], v[:, : 3 * tokens]], axis=1),
        lambda v: jnp.concatenate([v[:, tokens:], v[:, :tokens]], axis=1),
    )
    hidden = jax.nn.gelu(hidden_sum, approximate=False).astype(BF)
    hidden_all = jnp.concatenate(gather_tp(hidden), axis=0)
    down_terms = jnp.stack(
        [
            lax.dot_general(hidden_all, down_weight[i], (((0,), (0,)), ((), ())), preferred_element_type=F32).astype(BF)
            for i in range(2)
        ]
    )
    groups = [down_terms[:, g * tokens : (g + 1) * tokens] for g in (0, 3, 2, 1)]
    merged_halves = reduce_ring(groups, "x").astype(BF)
    merged = jnp.concatenate([merged_halves[0], merged_halves[1]], axis=1)

    owner_count = 16
    pair_cap = 2 * tokens // owner_count
    destination = owners[:, 0]
    owner_iota = jnp.arange(owner_count, dtype=jnp.int32)
    grid_counts = (destination[:, None] == owner_iota[None, :]).astype(jnp.int32).reshape(owner_count, tokens, -1)
    my_destination = lax.dynamic_slice_in_dim(destination, seq_index * tokens, tokens)
    earlier = token_at[None, :] < token_at[:, None]
    local_rank = jnp.sum(((my_destination[:, None] == my_destination[None, :]) & earlier).astype(jnp.int32), axis=1)
    send_index = my_destination * pair_cap + local_rank
    send_pick = (jnp.arange(owner_count * pair_cap, dtype=jnp.int32)[:, None] == send_index[None, :]).astype(BF)
    from_each = jnp.sum((destination.reshape(owner_count, tokens) == seq_index).astype(jnp.int32), axis=1)
    lower = owner_iota[None, :] < owner_iota[:, None]
    offsets = jnp.sum(jnp.where(lower, from_each[None, :], 0), axis=1)
    pair_rank = jnp.arange(pair_cap, dtype=jnp.int32)
    slot_count = text_embed.shape[0]
    placement = jnp.where(
        pair_rank[None, :] < from_each[:, None], offsets[:, None] + pair_rank[None, :], slot_count
    ).reshape(-1)
    slot_at = jnp.arange(slot_count, dtype=jnp.int32)
    is_vision = slot_at < jnp.sum(from_each)

    def route(rows):
        outgoing = jnp.dot(send_pick, rows, preferred_element_type=F32).astype(BF)
        arrived = lax.all_to_all(
            outgoing.reshape(owner_count, pair_cap, -1), seq, split_axis=0, concat_axis=0, tiled=True
        )
        return arrived.reshape(owner_count * pair_cap, -1)

    merged_in = route(merged)
    qkv_in = route(language_rows(merged))
    spread = (slot_at[:, None] == placement[None, :]).astype(BF)
    filled = jnp.where(
        is_vision[:, None], jnp.dot(spread, merged_in, preferred_element_type=F32), text_embed.astype(F32)
    )
    lang_attended = pl.pallas_call(
        language_kernel,
        out_shape=jax.ShapeDtypeStruct((slot_count, l_query.shape[1]), BF),
    )(
        qkv_in, text_qkv, placement[None, :], is_vision.astype(jnp.int32)[:, None],
        segment_ids[:, None], segment_ids[None, :],
    )

    width = text_embed.shape[1]
    steps = jnp.arange(4, dtype=jnp.int32)
    theirs = column_blocks(lang_attended, l_out, 2 * ((z + steps) % 4) + 1 - c, width)
    ours = column_blocks(lang_attended, l_out, 2 * ((z + steps) % 4) + c, width)
    summed = {}
    for d in (2, 1, 3, 0):
        summed[d] = ours[d].astype(F32) + shift(theirs[d], "c", 1).astype(F32)
    total = reduce_ring([summed[d] for d in range(4)], "z")
    return (filled + total).astype(BF)


def solution(mesh):
    fine = Mesh(mesh.devices.reshape(4, 4, 4, 2), ("x", "y", "z", "c"))
    seq, tp = ("x", "y"), ("z", "c")
    in_specs = (
        P(seq, None), P(), P(), P(None, tp), P(None, tp), P(None, tp), P(tp, None), P(), P(seq, tp), P(tp, seq),
        P(), P(seq, tp), P(seq), P(), P(None, tp), P(None, tp), P(None, tp), P(tp, None),
    )
    return jax.shard_map(body, mesh=fine, in_specs=in_specs, out_specs=P(seq, tp), check_vma=False)
```

```python
import math

import jax
import jax.numpy as jnp
from jax import lax
from jax.experimental import pallas as pl
from jax.experimental.pallas import tpu as pltpu
from jax.sharding import Mesh
from jax.sharding import PartitionSpec as P

DV = 1280
VHEADS = 16
D = 8192
LHD = 128
HEAD = DV // VHEADS
EPSILON = 1e-06
NEG_FILL = -1e30
BF = jnp.bfloat16
F32 = jnp.float32


def shift(value, axis, step):
    count = lax.axis_size(axis)
    return lax.ppermute(value, axis, [(i, (i + step) % count) for i in range(count)])


def after(value, other):
    return lax.optimization_barrier((value, other))[0]


def gather_direct(value, axis):
    return [value] + [shift(value, axis, d) for d in (1, 2, 3)]


def with_other_core(values):
    blocks = []
    for block in values:
        blocks += [block, shift(block, "c", 1)]
    return blocks


def reduce_direct(blocks, axis):
    total = blocks[0].astype(F32)
    for d in (1, 2, 3):
        total = total + shift(blocks[d], axis, d).astype(F32)
    return total


def reduce_ring(blocks, axis):
    half = blocks[2].shape[0] // 2
    up = shift(blocks[2][:half].astype(BF), axis, 1)
    down = shift(blocks[2][half:].astype(BF), axis, -1)
    nxt = jnp.concatenate([blocks[1][:half].astype(F32) + up.astype(F32), blocks[1][half:].astype(F32)], axis=0)
    prv = jnp.concatenate([blocks[3][:half].astype(F32), blocks[3][half:].astype(F32) + down.astype(F32)], axis=0)
    got = shift(nxt.astype(BF), axis, 1)
    got2 = shift(prv.astype(BF), axis, -1)
    return blocks[0].astype(F32) + got.astype(F32) + got2.astype(F32)


def rms_scaled(values, norm_gain):
    mean_square = jnp.mean(values * values, axis=-1, keepdims=True)
    return (values * lax.rsqrt(mean_square + EPSILON) * norm_gain).astype(BF)


def project_kernel(x_ref, gain_ref, wq_ref, wk_ref, wv_ref, kv_ref, q_ref):
    normed = rms_scaled(x_ref[...].astype(F32), gain_ref[...])
    width = wq_ref.shape[0]

    def project(weight):
        return lax.dot_general(weight, normed, (((1,), (1,)), ((), ())), preferred_element_type=F32).astype(BF)

    kv_ref[:width] = project(wk_ref[...])
    kv_ref[width:] = project(wv_ref[...])
    q_ref[...] = project(wq_ref[...])


def vision_kernel(pos_ref, q_ref, own_ref, left_ref, right_ref, qid_ref, kid_ref, out_ref):
    rows, count = q_ref.shape
    tokens = count // 4
    column = lax.broadcasted_iota(jnp.int32, (count, count), 1)
    source = lax.broadcasted_iota(jnp.int32, (count, count), 0)
    wanted = 4 * (column % tokens) + (column // tokens + pos_ref[0]) % 4
    order = (source == wanted).astype(F32).astype(BF)
    queries = jnp.dot(q_ref[...], order, preferred_element_type=F32).astype(BF)
    keys = jnp.concatenate([own_ref[:rows], left_ref[:rows], right_ref[:rows]], axis=1)
    values = jnp.concatenate([own_ref[rows:], left_ref[rows:], right_ref[rows:]], axis=1)
    wide = count // 2
    allowed = kid_ref[...] == qid_ref[...]
    scale = 1.0 / math.sqrt(HEAD)
    for part in range(2):
        for head in range(rows // HEAD):
            lower = head * HEAD
            scores = lax.dot_general(
                keys[lower : lower + HEAD],
                queries[lower : lower + HEAD, part * wide : (part + 1) * wide],
                (((0,), (0,)), ((), ())),
                preferred_element_type=F32,
            )
            scores = jnp.where(allowed, scores * scale, NEG_FILL)
            highest = jnp.max(scores, axis=0, keepdims=True)
            weights = jnp.where(allowed, jnp.exp(scores - highest), 0.0)
            totals = jnp.sum(weights, axis=0, keepdims=True)
            mixed = jnp.dot(values[lower : lower + HEAD], weights.astype(BF), preferred_element_type=F32)
            mixed = (mixed / totals).astype(BF)
            for i in range(2):
                out_ref[2 * part + i, lower : lower + HEAD] = mixed[:, i * tokens : (i + 1) * tokens]


def merge_kernel(pos_ref, *refs):
    att, weights, rest, (gain_ref, *ups), (out_ref, att_s, w_s, up_s, t_s) = (
        refs[:8], refs[8:16], refs[16:20], refs[20:25], refs[25:]
    )
    part, tokens = att[0].shape[0], rest[0].shape[0]
    for i in range(8):
        att_s[i * part : (i + 1) * part] = att[i][...]
        w_s[i * part : (i + 1) * part] = weights[i][...]
    rows = ups[0].shape[0]
    for d in range(4):
        start = pl.multiple_of((pos_ref[1] + 4 - d) % 4 * rows, rows)
        up_s[pl.ds(start, rows)] = ups[d][...]
    state = lax.dot_general(att_s[...], w_s[...], (((0,), (0,)), ((), ())), preferred_element_type=F32)
    state = state + jnp.concatenate([r[...] for r in rest], axis=0).astype(F32)
    normed = rms_scaled(state, gain_ref[...])
    t_s[...] = jnp.dot(normed, up_s[...], preferred_element_type=F32).T.astype(BF)
    for e in range(4):
        start = pl.multiple_of((pos_ref[0] + e) % 4 * part, part)
        term = t_s[pl.ds(start, part)]
        for d in range(4):
            g = (d + e) % 4
            out_ref[e, :, g * tokens : (g + 1) * tokens] = term[:, d * tokens : (d + 1) * tokens]


def down_kernel(pos_ref, *refs):
    hidden, parts, (out_ref, h_s, w_s) = refs[:8], refs[8:12], refs[12:]
    x, y, z, c = (pos_ref[i] for i in range(4))
    part, tokens = hidden[0].shape[0], out_ref.shape[1]
    for i in range(8):
        h_s[i * part : (i + 1) * part] = hidden[i][...]
    for d in range(4):
        back = (z - y + d + 4) % 4
        for k in range(4):
            slot = (x + 4 - k) % 4
            w_s[slot % 2 * 8 + 2 * back + (slot // 2 + 2 - c) % 2] = parts[d][k]
    width = w_s.shape[2]
    for b in range(2):
        right = w_s[8 * b : 8 * (b + 1)].reshape(8 * part, width)
        both = lax.dot_general(h_s[...], right, (((0,), (0,)), ((), ())), preferred_element_type=F32).astype(BF)
        for g in range(4):
            out_ref[(4 - g) % 4, :, b * width : (b + 1) * width] = both[g * tokens : (g + 1) * tokens]


def rows_kernel(order_ref, *refs, routed):
    blocks, (gain_ref, wq, wk, wv), rest = refs[:8], refs[8:12], refs[12:]
    (send_ref, out_ref, s, scale_s, acc) = rest if routed else (None, *rest)
    step = pl.program_id(0)

    @pl.when(step == 0)
    def _():
        total = jnp.zeros((s.shape[1], 1), F32)
        for i in range(8):
            s[i] = blocks[i][...]
            value = blocks[i][...].astype(F32)
            total = total + jnp.sum(value * value, axis=-1, keepdims=True)
        scale_s[...] = lax.rsqrt(total / D + EPSILON)
        acc[...] = jnp.zeros_like(acc)

    normed = (s[step].astype(F32) * scale_s[...] * gain_ref[...]).astype(BF)
    at = 0
    for weight in (wq, wk, wv):
        width = weight.shape[1]
        acc[:, at : at + width] += jnp.dot(normed, weight[...], preferred_element_type=F32)
        at += width

    @pl.when(step == 7)
    def _():
        if routed:
            count = out_ref.shape[0]
            rows = s.shape[1]
            pick = (lax.broadcasted_iota(jnp.int32, (count, rows), 0) == send_ref[...]).astype(F32).astype(BF)
            out_ref[:, :at] = jnp.dot(pick, acc[...].astype(BF), preferred_element_type=F32).astype(BF)
            out_ref[:, at:] = jnp.dot(pick, s[0], preferred_element_type=F32).astype(BF)
        else:
            out_ref[...] = acc[...].astype(BF)


def language_rows(order, blocks, gain, weights, send=None):
    rows, width = blocks[0].shape
    total = sum(w.shape[1] for w in weights)
    whole = lambda shape: pl.BlockSpec(shape, lambda i, o: (0, 0))
    specs = [whole((rows, width))] * 8 + [pl.BlockSpec((1, width), lambda i, o: (0, o[i]))]
    specs += [pl.BlockSpec((width, w.shape[1]), lambda i, o: (o[i], 0)) for w in weights]
    operands = [*blocks, gain[None, :], *weights]
    shape = (rows, total)
    if send is not None:
        specs.append(whole(send.shape))
        operands.append(send)
        shape = (2 * rows, total + width)
    return pl.pallas_call(
        lambda *refs: rows_kernel(*refs, routed=send is not None),
        grid_spec=pltpu.PrefetchScalarGridSpec(
            num_scalar_prefetch=1,
            grid=(8,),
            in_specs=specs,
            out_specs=whole(shape),
            scratch_shapes=[
                pltpu.VMEM((8, rows, width), BF),
                pltpu.VMEM((rows, 1), F32),
                pltpu.VMEM((rows, total), F32),
            ],
        ),
        out_shape=jax.ShapeDtypeStruct(shape, BF),
        name="rows_kernel",
    )(order, *operands)


def language_kernel(in_ref, text_ref, embed_ref, place_ref, vis_ref, sega_ref, segb_ref, out_ref, filled_ref):
    slots, features = text_ref.shape
    row = lax.broadcasted_iota(jnp.int32, (slots, slots), 0)
    col = lax.broadcasted_iota(jnp.int32, (slots, slots), 1)
    spread = (row == place_ref[...]).astype(F32).astype(BF)
    visual = vis_ref[...] > 0
    placed = jnp.dot(spread, in_ref[:, :features], preferred_element_type=F32)
    qkv = jnp.where(visual, placed, text_ref[...].astype(F32)).astype(BF)
    placed = jnp.dot(spread, in_ref[:, features:], preferred_element_type=F32)
    filled_ref[...] = jnp.where(visual, placed, embed_ref[...].astype(F32)).astype(BF)
    allowed = (sega_ref[...] == segb_ref[...]) & (col <= row)
    width = out_ref.shape[1]
    keys, values = qkv[:, width : width + LHD], qkv[:, width + LHD :]
    for head in range(width // LHD):
        scores = lax.dot_general(
            qkv[:, head * LHD : (head + 1) * LHD], keys, (((1,), (1,)), ((), ())), preferred_element_type=F32
        ) * (1.0 / math.sqrt(LHD))
        scores = jnp.where(allowed, scores, NEG_FILL)
        highest = jnp.max(scores, axis=-1, keepdims=True)
        weights = jnp.where(allowed, jnp.exp(scores - highest), 0.0)
        totals = jnp.sum(weights, axis=-1, keepdims=True)
        mixed = jnp.dot(weights.astype(BF), values, preferred_element_type=F32)
        out_ref[:, head * LHD : (head + 1) * LHD] = (mixed / totals).astype(BF)


def blocks_kernel(order_ref, mine_ref, theirs_ref, right_ref, other_ref, out_ref):
    out_ref[0] = (
        jnp.dot(mine_ref[...], right_ref[...], preferred_element_type=F32)
        + jnp.dot(theirs_ref[...], other_ref[0], preferred_element_type=F32)
    ).astype(BF)


def column_blocks(mine, theirs, right, other, order, width):
    count = order.shape[0]
    return pl.pallas_call(
        blocks_kernel,
        grid_spec=pltpu.PrefetchScalarGridSpec(
            num_scalar_prefetch=1,
            grid=(count,),
            in_specs=[
                pl.BlockSpec(mine.shape, lambda i, o: (0, 0)),
                pl.BlockSpec(mine.shape, lambda i, o: (0, 0)),
                pl.BlockSpec((right.shape[0], width), lambda i, o: (0, o[i])),
                pl.BlockSpec((1, right.shape[0], width), lambda i, o: (o[i] // 2, 0, 0)),
            ],
            out_specs=pl.BlockSpec((1, mine.shape[0], width), lambda i, o: (i, 0, 0)),
        ),
        out_shape=jax.ShapeDtypeStruct((count, mine.shape[0], width), BF),
    )(order, mine, theirs, right, other)


def body(
    patches, image_ids, vision_gain, v_query, v_key, v_value, v_out, merge_gain, merge_up, merge_down,
    owners, text_embed, segment_ids, lang_gain, l_query, l_key, l_value, l_out,
):
    x, y, z, c = (lax.axis_index(a) for a in ("x", "y", "z", "c"))
    seq_index = 4 * x + y
    row_count = patches.shape[0]
    tokens = row_count // 4
    local = v_query.shape[1]

    pos = jnp.stack([x, y, z, c]).astype(jnp.int32)
    scalars = pl.BlockSpec(memory_space=pltpu.SMEM)
    vmem = pl.BlockSpec(memory_space=pltpu.VMEM)

    key_value, query_own = pl.pallas_call(
        project_kernel,
        out_shape=[
            jax.ShapeDtypeStruct((2 * local, row_count), BF),
            jax.ShapeDtypeStruct((local, row_count), BF),
        ],
        name="project_kernel",
    )(patches, vision_gain[None, :], v_query.T, v_key.T, v_value.T)
    seq = ("x", "y")
    with jax.named_scope("halo"):
        left, right = shift(key_value, seq, 1), shift(key_value, seq, -1)
    padded_ids = jnp.pad(image_ids, (tokens, tokens), constant_values=-1)
    near_ids = lax.dynamic_slice_in_dim(padded_ids, seq_index * tokens, 3 * tokens)
    own_ids = near_ids[tokens : 2 * tokens]
    key_ids = jnp.repeat(near_ids, 4)
    left_ids, mid_ids, right_ids = (key_ids[i * row_count : (i + 1) * row_count] for i in range(3))
    attended = pl.pallas_call(
        vision_kernel,
        in_specs=[scalars] + [vmem] * 6,
        out_specs=vmem,
        out_shape=jax.ShapeDtypeStruct((4, local, tokens), BF),
        name="vision_kernel",
    )(
        pos, query_own, key_value, left, right,
        jnp.tile(own_ids, 2)[None, :],
        jnp.concatenate([mid_ids, left_ids, right_ids])[:, None],
    )

    token_at = jnp.arange(tokens, dtype=jnp.int32)
    patch_at = jnp.arange(row_count, dtype=jnp.int32)
    wanted = 4 * (patch_at % tokens) + (patch_at // tokens + x) % 4
    with jax.named_scope("early"):
        out_blocks = gather_direct(after(v_out, query_own), "z")
        picked = jnp.dot(
            (patch_at[None, :] == wanted[:, None]).astype(BF), after(patches, query_own), preferred_element_type=F32
        ).astype(BF)
        picked = [picked[d * tokens : (d + 1) * tokens] for d in range(4)]
        residual = [picked[0]] + [shift(picked[d], "x", d) for d in (1, 2, 3)]

    with jax.named_scope("swap"):
        att_moved = [attended[0]] + [shift(attended[d], "x", d) for d in (1, 2, 3)]
    with jax.named_scope("second"):
        up_blocks = gather_direct(after(merge_up, attended), "y")
        yh, b = y // 2, y % 2
        down_parts = after(merge_down, attended).reshape(4, merge_down.shape[0] // 4, -1)
        moved = []
        for k in range(4):
            pairs = []
            for sx in range(4):
                for sy in range(4):
                    for sz in range(4):
                        for sc in range(2):
                            to = (2 * sc + sy % 2 + k) % 4
                            pairs.append((((sx * 4 + sy) * 4 + sz) * 2 + sc, ((to * 4 + sz) * 4 + sx) * 2 + sy // 2))
            part = lax.dynamic_index_in_dim(down_parts, (2 * c + b + k) % 4, 0, keepdims=False)
            moved.append(lax.ppermute(part, ("x", "y", "z", "c"), pairs))
        down_own = jnp.stack(moved)
    att_rows = jnp.concatenate(att_moved, axis=1)
    with jax.named_scope("gather_att"):
        att_all = with_other_core(gather_direct(att_rows, "z"))
    out_all = with_other_core([after(w, att_rows) for w in out_blocks])
    up_terms = pl.pallas_call(
        merge_kernel,
        in_specs=[scalars] + [vmem] * 25,
        out_specs=vmem,
        out_shape=jax.ShapeDtypeStruct((4, local, row_count), BF),
        scratch_shapes=[
            pltpu.VMEM((8 * local, row_count), BF),
            pltpu.VMEM((8 * local, DV), BF),
            pltpu.VMEM((4 * merge_up.shape[0], merge_up.shape[1]), BF),
            pltpu.VMEM((4 * local, row_count), BF),
        ],
        name="merge_kernel",
    )(pos, *att_all, *out_all, *residual, merge_gain[None, :], *up_blocks)
    with jax.named_scope("sum_up"):
        hidden_sum = reduce_direct([up_terms[e] for e in range(4)], "x")
    hidden = jax.nn.gelu(hidden_sum, approximate=False).astype(BF)
    text_half = text_embed.shape[0] // 2
    with jax.named_scope("third"):
        text_own = after(text_embed, up_terms)
        text_before, text_behind = shift(text_own, "z", 1), shift(text_own, "z", -1)
        down_blocks = gather_direct(after(down_own, up_terms), "y")
    with jax.named_scope("gather_hidden"):
        hidden_all = with_other_core(gather_direct(hidden, "z"))
    down_terms = pl.pallas_call(
        down_kernel,
        in_specs=[scalars] + [vmem] * 12,
        out_specs=vmem,
        out_shape=jax.ShapeDtypeStruct((4, tokens, 2 * merge_down.shape[1]), BF),
        scratch_shapes=[
            pltpu.VMEM((8 * local, row_count), BF),
            pltpu.VMEM((16, merge_down.shape[0] // 4, merge_down.shape[1]), BF),
        ],
        name="down_kernel",
    )(pos, *hidden_all, *down_blocks)
    with jax.named_scope("sum_down"):
        merged = reduce_direct([down_terms[e] for e in range(4)], "x").astype(BF)
    l_width = text_embed.shape[1]
    with jax.named_scope("fourth"):
        text_low = shift(after(text_before, down_terms)[:text_half], "z", 1)
        text_high = shift(after(text_behind, down_terms)[text_half:], "z", -1)
        text_far = jnp.concatenate([text_low, text_high], axis=0)
        out_cols = after(l_out, down_terms)
        other_out = shift(
            jnp.stack([lax.dynamic_slice_in_dim(out_cols, (2 * i + 1 - c) * l_width, l_width, 1) for i in range(4)]),
            "c",
            1,
        )
    with jax.named_scope("gather_merged"):
        merged_blocks = with_other_core(gather_direct(merged, "z"))
    text_blocks = with_other_core([after(v, merged) for v in (text_own, text_before, text_far, text_behind)])
    block_order = jnp.stack(
        [2 * ((z + 4 - r) % 4) + (c + other) % 2 for r in range(4) for other in range(2)]
    ).astype(jnp.int32)
    projections = (l_query, l_key, l_value)
    text_qkv = language_rows(block_order, text_blocks, lang_gain, projections)

    owner_count = 16
    pair_cap = 2 * tokens // owner_count
    destination = owners[:, 0]
    owner_iota = jnp.arange(owner_count, dtype=jnp.int32)
    my_destination = lax.dynamic_slice_in_dim(destination, seq_index * tokens, tokens)
    earlier = token_at[None, :] < token_at[:, None]
    local_rank = jnp.sum(((my_destination[:, None] == my_destination[None, :]) & earlier).astype(jnp.int32), axis=1)
    send_index = my_destination * pair_cap + local_rank
    from_each = jnp.sum((destination.reshape(owner_count, tokens) == seq_index).astype(jnp.int32), axis=1)
    lower = owner_iota[None, :] < owner_iota[:, None]
    offsets = jnp.sum(jnp.where(lower, from_each[None, :], 0), axis=1)
    pair_rank = jnp.arange(pair_cap, dtype=jnp.int32)
    slot_count = text_embed.shape[0]
    placement = jnp.where(
        pair_rank[None, :] < from_each[:, None], offsets[:, None] + pair_rank[None, :], slot_count
    ).reshape(-1)
    slot_at = jnp.arange(slot_count, dtype=jnp.int32)
    is_vision = slot_at < jnp.sum(from_each)


    outgoing = language_rows(block_order, merged_blocks, lang_gain, projections, send_index[None, :])
    incoming = lax.all_to_all(
        outgoing.reshape(owner_count, pair_cap, -1), seq, split_axis=0, concat_axis=0, tiled=True
    ).reshape(owner_count * pair_cap, -1)
    lang_attended, filled = pl.pallas_call(
        language_kernel,
        out_shape=[
            jax.ShapeDtypeStruct((slot_count, l_query.shape[1]), BF),
            jax.ShapeDtypeStruct(text_embed.shape, BF),
        ],
        name="language_kernel",
    )(
        incoming, text_qkv, text_embed, placement[None, :], is_vision.astype(jnp.int32)[:, None],
        segment_ids[:, None], segment_ids[None, :],
    )

    order = (2 * ((z + jnp.array([2, 1, 3, 0], dtype=jnp.int32)) % 4) + c).astype(jnp.int32)
    terms = column_blocks(lang_attended, shift(lang_attended, "c", 1), l_out, other_out, order, l_width)
    total = reduce_ring([terms[3], terms[1], terms[0], terms[2]], "z")
    return (filled.astype(F32) + total).astype(BF)


def solution(mesh):
    fine = Mesh(mesh.devices.reshape(4, 4, 4, 2), ("x", "y", "z", "c"))
    seq, tp = ("x", "y"), ("z", "c")
    in_specs = (
        P(seq, None), P(), P(), P(None, tp), P(None, tp), P(None, tp), P(tp, None), P(), P(seq, tp), P(tp, seq),
        P(), P(seq, tp), P(seq), P(), P(None, tp), P(None, tp), P(None, tp), P(tp, None),
    )
    return jax.shard_map(body, mesh=fine, in_specs=in_specs, out_specs=P(seq, tp), check_vma=False)
```

```python
import math

import jax
import jax.numpy as jnp
from jax import lax
from jax.experimental import pallas as pl
from jax.experimental.pallas import tpu as pltpu
from jax.sharding import Mesh
from jax.sharding import PartitionSpec as P

DV = 1280
VHEADS = 16
D = 8192
LHD = 128
HEAD = DV // VHEADS
EPSILON = 1e-06
NEG_FILL = -1e30
BF = jnp.bfloat16
F32 = jnp.float32


def shift(value, axis, step):
    count = lax.axis_size(axis)
    return lax.ppermute(value, axis, [(i, (i + step) % count) for i in range(count)])


def after(value, other):
    return lax.optimization_barrier((value, other))[0]


def limit(mebibytes):
    return pltpu.CompilerParams(vmem_limit_bytes=mebibytes << 20)


def gather_direct(value, axis):
    return [value] + [shift(value, axis, d) for d in (1, 2, 3)]


def gather_halves(value, axis):
    half = value.shape[0] // 2
    before, behind = shift(value, axis, 1), shift(value, axis, -1)
    low, high = shift(before[:half], axis, 1), shift(behind[half:], axis, -1)
    return [value, before, behind, low, high]


def swap_cores(value):
    return shift(value, "c", 1)


def reduce_direct(blocks, axis):
    total = blocks[0].astype(F32)
    for d in (1, 2, 3):
        total = total + shift(blocks[d], axis, d).astype(F32)
    return total


def rms_scaled(values, norm_gain):
    mean_square = jnp.mean(values * values, axis=-1, keepdims=True)
    return (values * lax.rsqrt(mean_square + EPSILON) * norm_gain).astype(BF)


def project_kernel(pos_ref, x_ref, gain_ref, wq_ref, wk_ref, wv_ref, down_ref, kv_ref, q_ref, *rest):
    normed = rms_scaled(x_ref[...].astype(F32), gain_ref[...][None, :])
    width = wq_ref.shape[0]

    def project(weight):
        return lax.dot_general(weight, normed, (((1,), (1,)), ((), ())), preferred_element_type=F32).astype(BF)

    kv_ref[:width] = project(wk_ref[...])
    kv_ref[width:] = project(wv_ref[...])
    q_ref[...] = project(wq_ref[...])
    picked, quarters = rest[:4], rest[4:]
    narrow = quarters[0].shape[1]
    for e in range(4):
        start = pl.multiple_of((pos_ref[2] + e) % 4 * narrow, narrow)
        quarters[e][...] = down_ref[:, pl.ds(start, narrow)]
    count = x_ref.shape[0]
    for d in range(4):
        tokens = picked[d].shape[0]
        token = lax.broadcasted_iota(jnp.int32, (tokens, count), 0) + (pos_ref[3] * tokens if d else 0)
        patch = lax.broadcasted_iota(jnp.int32, (tokens, count), 1)
        pick = (patch == 4 * token + (pos_ref[0] + d) % 4).astype(F32).astype(BF)
        picked[d][...] = jnp.dot(pick, x_ref[...], preferred_element_type=F32).astype(BF)


def vision_kernel(pos_ref, q_ref, own_ref, left_ref, right_ref, qid_ref, kid_ref, *refs):
    outs, (queries_s, keys_s, values_s, mixed_s) = refs[:4], refs[4:]
    rows, count = q_ref.shape
    tokens, wide = count // 4, count // 2
    column = lax.broadcasted_iota(jnp.int32, (count, count), 1)
    source = lax.broadcasted_iota(jnp.int32, (count, count), 0)
    wanted = 4 * (column % tokens) + (column // tokens + pos_ref[0]) % 4
    order = (source == wanted).astype(F32).astype(BF)
    queries = jnp.dot(q_ref[...], order, preferred_element_type=F32).astype(BF)
    for part in range(2):
        queries_s[part] = queries[:, part * wide : (part + 1) * wide]
    for i, ref in enumerate((own_ref, left_ref, right_ref)):
        keys_s[:, i * count : (i + 1) * count] = ref[:rows]
        values_s[:, i * count : (i + 1) * count] = ref[rows:]
    allowed = kid_ref[...] == qid_ref[...]
    scale = 1.0 / math.sqrt(HEAD)

    def one(step, _):
        lower = pl.multiple_of(step // 2 * HEAD, HEAD)
        scores = lax.dot_general(
            keys_s[pl.ds(lower, HEAD)], queries_s[step % 2, pl.ds(lower, HEAD)],
            (((0,), (0,)), ((), ())), preferred_element_type=F32,
        )
        scores = jnp.where(allowed, scores * scale, NEG_FILL)
        highest = jnp.max(scores, axis=0, keepdims=True)
        weights = jnp.where(allowed, jnp.exp(scores - highest), 0.0)
        totals = jnp.sum(weights, axis=0, keepdims=True)
        mixed = jnp.dot(values_s[pl.ds(lower, HEAD)], weights.astype(BF), preferred_element_type=F32)
        mixed_s[step % 2, pl.ds(lower, HEAD)] = (mixed / totals).astype(BF)
        return 0

    lax.fori_loop(0, 2 * (rows // HEAD), one, 0)
    for i in range(4):
        outs[i][...] = mixed_s[i // 2, :, i % 2 * tokens : (i % 2 + 1) * tokens]


def merge_kernel(pos_ref, *refs):
    att, weights, rest, (gain_ref, *ups), outs, (att_s, w_s, up_s, t_s, rest_s) = (
        refs[:8], refs[8:18], refs[18:25], refs[25:31], refs[31:35], refs[35:]
    )
    part, tokens = att[0].shape[0], rest[0].shape[0]
    for i in range(8):
        att_s[i * part : (i + 1) * part] = att[i][...]
    for other in range(2):
        own, before, behind, low, high = weights[5 * other : 5 * other + 5]
        for r, ref in ((0, own), (1, before), (3, behind)):
            start = (2 * r + other) * part
            w_s[start : start + part] = ref[...]
        start = (4 + other) * part
        w_s[start : start + part // 2] = low[...]
        w_s[start + part // 2 : start + part] = high[...]
    rows = ups[0].shape[0]
    for d, offset, ref in ((0, 0, ups[0]), (1, 0, ups[1]), (3, 0, ups[2]), (2, 0, ups[3]), (2, rows // 2, ups[4])):
        start = pl.multiple_of((pos_ref[1] + 4 - d) % 4 * rows + offset, rows // 2)
        up_s[pl.ds(start, ref.shape[0])] = ref[...]
    rest_s[:tokens] = rest[0][...]
    for d in range(1, 4):
        for other in range(2):
            start = pl.multiple_of(d * tokens + (pos_ref[3] + other) % 2 * (tokens // 2), tokens // 2)
            rest_s[pl.ds(start, tokens // 2)] = rest[2 * d - 1 + other][...]
    state = lax.dot_general(att_s[...], w_s[...], (((0,), (0,)), ((), ())), preferred_element_type=F32)
    state = state + rest_s[...].astype(F32)
    normed = rms_scaled(state, gain_ref[...][None, :])
    t_s[...] = jnp.dot(normed, up_s[...], preferred_element_type=F32).T.astype(BF)
    for e in range(4):
        start = pl.multiple_of((pos_ref[0] + e) % 4 * part, part)
        term = t_s[pl.ds(start, part)]
        for d in range(4):
            g = (d + e) % 4
            outs[e][:, g * tokens : (g + 1) * tokens] = term[:, d * tokens : (d + 1) * tokens]


def regroup_kernel(pos_ref, *refs):
    blocks, outs = refs[:4], refs[4:]
    part = blocks[0].shape[0] // 4
    for e in range(4):
        start = pl.multiple_of((pos_ref[0] + e) % 4 * part, part)
        for r in range(4):
            outs[e][r * part : (r + 1) * part] = blocks[r][pl.ds(start, part)]


def down_kernel(pos_ref, *refs):
    hidden, parts, outs, (h_s, w_s) = refs[:8], refs[8:18], refs[18:22], refs[22:]
    x, y, c = pos_ref[0], pos_ref[1], pos_ref[3]
    part, tokens = hidden[0].shape[0], outs[0].shape[0]
    narrow = parts[0].shape[2]
    for i in range(8):
        h_s[i * part : (i + 1) * part] = hidden[i][...]

    def place(ref, other, d, first):
        for q in range(ref.shape[0]):
            at = (x + 4 - first - q) % 4 * 2 + (y + 4 - d) % 4 // 2
            column = pl.ds(pl.multiple_of(at * narrow, narrow), narrow)
            for r in range(4):
                start = (2 * r + other) * part
                w_s[start : start + part, column] = ref[q, r * part : (r + 1) * part]

    @pl.when((y + c) % 2 == 0)
    def _():
        for other in range(2):
            place(parts[5 * other], other, 0, 0)
            place(parts[5 * other + 3], other, 2, 0)
            place(parts[5 * other + 4], other, 2, 2)

    @pl.when((y + c) % 2 == 1)
    def _():
        for other in range(2):
            place(parts[5 * other + 1], other, 1, 0)
            place(parts[5 * other + 2], other, 3, 0)

    both = lax.dot_general(h_s[...], w_s[...], (((0,), (0,)), ((), ())), preferred_element_type=F32).astype(BF)
    for g in range(4):
        outs[(4 - g) % 4][...] = both[g * tokens : (g + 1) * tokens]


def rows_kernel(pos_ref, *refs, routed):
    count = 8 if routed else 10
    blocks, (gain_ref, *weights), rest = refs[:count], refs[count : count + 4], refs[count + 4 :]
    (send_ref, out_ref, own_ref, s, *buffers, sems) = rest if routed else (None, rest[0], None, *rest[1:])
    rows, width = s.shape[0], s.shape[1] // 8
    z, c = pos_ref[2], pos_ref[3]

    def copies(i):
        start = i * width if isinstance(i, int) else pl.multiple_of(i * width, width)
        return [
            pltpu.make_async_copy(weight.at[pl.ds(start, width)], buffer.at[i], sems.at[i, j])
            for j, (weight, buffer) in enumerate(zip(weights, buffers))
        ]

    for i in range(8):
        for copy in copies(i):
            copy.start()
    total = jnp.zeros((rows, 1), F32)
    if routed:
        narrow = width // 8
        for i in range(8):
            value = blocks[i][...].astype(F32)
            total = total + jnp.sum(value * value, axis=-1, keepdims=True)
            core = (c + i % 2) % 2
            for k in range(8):
                start = pl.multiple_of((core + 2 * k) * 4 * narrow + (z + 4 - i // 2) % 4 * narrow, narrow)
                s[:, pl.ds(start, narrow)] = blocks[i][:, k * narrow : (k + 1) * narrow]
    else:
        half = rows // 2
        for other in range(2):
            own, before, behind, low, high = blocks[5 * other : 5 * other + 5]
            for r, first, ref in ((0, 0, own), (1, 0, before), (3, 0, behind), (2, 0, low), (2, half, high)):
                start = pl.multiple_of((2 * ((z + 4 - r) % 4) + (c + other) % 2) * width, width)
                s[first : first + ref.shape[0], pl.ds(start, width)] = ref[...]
        for i in range(8):
            value = s[:, i * width : (i + 1) * width].astype(F32)
            total = total + jnp.sum(value * value, axis=-1, keepdims=True)
    scale = lax.rsqrt(total / D + EPSILON)

    def one(i, sums):
        for copy in copies(i):
            copy.wait()
        columns = pl.ds(pl.multiple_of(i * width, width), width)
        normed = (s[:, columns].astype(F32) * scale * gain_ref[:, columns]).astype(BF)
        return tuple(t + jnp.dot(normed, buffer[i], preferred_element_type=F32) for t, buffer in zip(sums, buffers))

    sums = lax.fori_loop(0, 8, one, tuple(jnp.zeros((rows, w.shape[1]), F32) for w in weights))
    whole = jnp.concatenate(sums, axis=1).astype(BF)
    if routed:
        pick = (lax.broadcasted_iota(jnp.int32, (out_ref.shape[0], rows), 0) == send_ref[...]).astype(F32).astype(BF)
        out_ref[...] = jnp.dot(pick, whole, preferred_element_type=F32).astype(BF)
        own = s[:, pl.ds(pl.multiple_of((2 * z + c) * width, width), width)]
        own_ref[...] = jnp.dot(pick, own, preferred_element_type=F32).astype(BF)
    else:
        out_ref[...] = whole


def language_rows(pos, blocks, gain, weights, send=None):
    rows, width = blocks[0].shape
    total = sum(w.shape[1] for w in weights)
    operands = [pos, *blocks, gain[None, :], *weights]
    vmem, hbm = pl.BlockSpec(memory_space=pltpu.VMEM), pl.BlockSpec(memory_space=pltpu.HBM)
    specs = [pl.BlockSpec(memory_space=pltpu.SMEM)] + [vmem] * (len(blocks) + 1) + [hbm] * 3
    shapes = [jax.ShapeDtypeStruct((rows, total), BF)]
    if send is not None:
        operands.append(send)
        specs.append(vmem)
        shapes = [jax.ShapeDtypeStruct((2 * rows, n), BF) for n in (total, width)]
    return pl.pallas_call(
        lambda *refs: rows_kernel(*refs, routed=send is not None),
        in_specs=specs,
        out_specs=[vmem] * len(shapes),
        out_shape=shapes,
        scratch_shapes=[pltpu.VMEM((rows, 8 * width), BF)]
        + [pltpu.VMEM((8, width, w.shape[1]), BF) for w in weights]
        + [pltpu.SemaphoreType.DMA((8, 3))],
        name="rows_kernel",
    )(*operands)


def fill_kernel(in_ref, embed_ref, place_ref, vis_ref, out_ref):
    slots = embed_ref.shape[0]
    spread = (lax.broadcasted_iota(jnp.int32, (slots, slots), 0) == place_ref[...]).astype(F32).astype(BF)
    placed = jnp.dot(spread, in_ref[...], preferred_element_type=F32)
    out_ref[...] = jnp.where(vis_ref[...] > 0, placed, embed_ref[...].astype(F32)).astype(BF)


def language_kernel(in_ref, text_ref, place_ref, vis_ref, sega_ref, segb_ref, out_ref):
    slots = text_ref.shape[0]
    row = lax.broadcasted_iota(jnp.int32, (slots, slots), 0)
    col = lax.broadcasted_iota(jnp.int32, (slots, slots), 1)
    spread = (row == place_ref[...]).astype(F32).astype(BF)
    visual = vis_ref[...] > 0
    placed = jnp.dot(spread, in_ref[...], preferred_element_type=F32)
    qkv = jnp.where(visual, placed, text_ref[...].astype(F32)).astype(BF)
    allowed = (sega_ref[...] == segb_ref[...]) & (col <= row)
    width = out_ref.shape[1]
    keys, values = qkv[:, width : width + LHD], qkv[:, width + LHD :]
    for head in range(width // LHD):
        scores = lax.dot_general(
            qkv[:, head * LHD : (head + 1) * LHD], keys, (((1,), (1,)), ((), ())), preferred_element_type=F32
        ) * (1.0 / math.sqrt(LHD))
        scores = jnp.where(allowed, scores, NEG_FILL)
        highest = jnp.max(scores, axis=-1, keepdims=True)
        weights = jnp.where(allowed, jnp.exp(scores - highest), 0.0)
        totals = jnp.sum(weights, axis=-1, keepdims=True)
        mixed = jnp.dot(weights.astype(BF), values, preferred_element_type=F32)
        out_ref[:, head * LHD : (head + 1) * LHD] = (mixed / totals).astype(BF)


def block_kernel(at_ref, mine_ref, theirs_ref, right_ref, other_ref, *refs):
    outs, (column_s, sem) = refs[:-2], refs[-2:]
    width = other_ref.shape[1]
    start = pl.multiple_of(at_ref[0] * width, width)
    copy = pltpu.make_async_copy(right_ref.at[:, pl.ds(start, width)], column_s, sem)
    copy.start()
    both = jnp.dot(theirs_ref[...], other_ref[...], preferred_element_type=F32)
    copy.wait()
    both = both + jnp.dot(mine_ref[...], column_s[...], preferred_element_type=F32)
    rows = outs[0].shape[0]
    for i, out in enumerate(outs):
        out[...] = both[i * rows : (i + 1) * rows].astype(BF)


def column_block(mine, theirs, right, other, block, count):
    width, rows = other.shape[1], mine.shape[0] // count
    vmem = pl.BlockSpec(memory_space=pltpu.VMEM)
    return pl.pallas_call(
        block_kernel,
        in_specs=[pl.BlockSpec(memory_space=pltpu.SMEM), vmem, vmem, pl.BlockSpec(memory_space=pltpu.HBM), vmem],
        out_specs=[vmem] * count,
        out_shape=[jax.ShapeDtypeStruct((rows, width), BF)] * count,
        scratch_shapes=[pltpu.VMEM(other.shape, BF), pltpu.SemaphoreType.DMA],
        name="block_kernel",
    )(block.reshape(1).astype(jnp.int32), mine, theirs, right, other)


def body(
    patches, image_ids, vision_gain, v_query, v_key, v_value, v_out, merge_gain, merge_up, merge_down,
    owners, text_embed, segment_ids, lang_gain, l_query, l_key, l_value, l_out,
):
    x, y, z, c = (lax.axis_index(a) for a in ("x", "y", "z", "c"))
    seq_index = 4 * x + y
    row_count = patches.shape[0]
    tokens = row_count // 4
    local = v_query.shape[1]

    pos = jnp.stack([x, y, z, c]).astype(jnp.int32)
    scalars = pl.BlockSpec(memory_space=pltpu.SMEM)
    vmem = pl.BlockSpec(memory_space=pltpu.VMEM)

    key_value, query_own, *cut = pl.pallas_call(
        project_kernel,
        in_specs=[scalars] + [vmem] * 6,
        out_specs=[vmem] * 10,
        out_shape=[
            jax.ShapeDtypeStruct((2 * local, row_count), BF),
            jax.ShapeDtypeStruct((local, row_count), BF),
        ]
        + [jax.ShapeDtypeStruct((tokens, DV), BF)]
        + [jax.ShapeDtypeStruct((tokens // 2, DV), BF)] * 3
        + [jax.ShapeDtypeStruct((merge_down.shape[0], merge_down.shape[1] // 4), BF)] * 4,
        name="project_kernel",
    )(pos, patches, vision_gain, v_query.T, v_key.T, v_value.T, merge_down)
    picked, quarters = cut[:4], cut[4:]
    seq = ("x", "y")
    left, right = shift(key_value, seq, 1), shift(key_value, seq, -1)
    padded_ids = jnp.pad(image_ids, (tokens, tokens), constant_values=-1)
    near_ids = lax.dynamic_slice_in_dim(padded_ids, seq_index * tokens, 3 * tokens)
    own_ids = near_ids[tokens : 2 * tokens]
    key_ids = jnp.repeat(near_ids, 4)
    left_ids, mid_ids, right_ids = (key_ids[i * row_count : (i + 1) * row_count] for i in range(3))
    attended = pl.pallas_call(
        vision_kernel,
        in_specs=[scalars] + [vmem] * 6,
        out_specs=[vmem] * 4,
        out_shape=[jax.ShapeDtypeStruct((local, tokens), BF)] * 4,
        scratch_shapes=[
            pltpu.VMEM((2, local, row_count // 2), BF),
            pltpu.VMEM((local, 3 * row_count), BF),
            pltpu.VMEM((local, 3 * row_count), BF),
            pltpu.VMEM((2, local, row_count // 2), BF),
        ],
        compiler_params=limit(24),
        name="vision_kernel",
    )(
        pos, query_own, key_value, left, right,
        jnp.tile(own_ids, 2)[None, :],
        jnp.concatenate([mid_ids, left_ids, right_ids])[:, None],
    )

    token_at = jnp.arange(tokens, dtype=jnp.int32)
    down_z = [quarters[0]] + [shift(quarters[e], "z", e) for e in (1, 2, 3)]
    out_parts = gather_halves(after(v_out, query_own), "z")

    att_moved = [attended[0]] + [shift(attended[d], "x", d) for d in (1, 2, 3)]
    up_parts = gather_halves(after(merge_up, attended[0]), "y")
    att_rows = jnp.concatenate(att_moved, axis=1)
    att_z = gather_direct(att_rows, "z")
    moved_patches = [shift(after(picked[d], attended[0]), "x", d) for d in (1, 2, 3)]
    residual = [picked[0]] + [v for p in moved_patches for v in (p, swap_cores(p))]
    att_all = [v for block in att_z for v in (block, swap_cores(block))]
    out_all = out_parts + [swap_cores(after(part, att_rows)) for part in out_parts]
    down_terms = pl.pallas_call(
        regroup_kernel,
        in_specs=[scalars] + [vmem] * 4,
        out_specs=[vmem] * 4,
        out_shape=[jax.ShapeDtypeStruct(quarters[0].shape, BF)] * 4,
        compiler_params=limit(8),
        name="regroup_kernel",
    )(pos, *[after(part, att_rows) for part in down_z])
    down_own = jnp.stack([down_terms[0]] + [shift(down_terms[e], "x", e) for e in (1, 2, 3)])
    up_terms = pl.pallas_call(
        merge_kernel,
        in_specs=[scalars] + [vmem] * 31,
        out_specs=[vmem] * 4,
        out_shape=[jax.ShapeDtypeStruct((local, row_count), BF)] * 4,
        scratch_shapes=[
            pltpu.VMEM((8 * local, row_count), BF),
            pltpu.VMEM((8 * local, DV), BF),
            pltpu.VMEM((4 * merge_up.shape[0], merge_up.shape[1]), BF),
            pltpu.VMEM((4 * local, row_count), BF),
            pltpu.VMEM((row_count, DV), BF),
        ],
        compiler_params=limit(32),
        name="merge_kernel",
    )(pos, *att_all, *out_all, *residual, merge_gain, *up_parts)
    hidden_sum = reduce_direct(up_terms, "x")
    hidden = jax.nn.gelu(hidden_sum, approximate=False).astype(BF)
    text_parts = gather_halves(after(text_embed, up_terms[0]), "z")
    down_parts = gather_halves(after(down_own, up_terms[0]), "y")
    hidden_z = gather_direct(hidden, "z")
    hidden_all = [v for block in hidden_z for v in (block, swap_cores(block))]
    down_all = down_parts + [swap_cores(part) for part in down_parts]
    down_terms = pl.pallas_call(
        down_kernel,
        in_specs=[scalars] + [vmem] * 18,
        out_specs=[vmem] * 4,
        out_shape=[jax.ShapeDtypeStruct((tokens, 2 * merge_down.shape[1]), BF)] * 4,
        scratch_shapes=[pltpu.VMEM((8 * local, row_count), BF), pltpu.VMEM((8 * local, 2 * merge_down.shape[1]), BF)],
        compiler_params=limit(24),
        name="down_kernel",
    )(pos, *hidden_all, *down_all)
    merged = reduce_direct(down_terms, "x").astype(BF)
    merged_z = gather_direct(merged, "z")
    merged_blocks = [v for block in merged_z for v in (block, swap_cores(block))]
    text_all = text_parts + [swap_cores(after(part, merged)) for part in text_parts]
    projections = (l_query, l_key, l_value)
    (text_qkv,) = language_rows(pos, text_all, lang_gain, projections)

    owner_count = 16
    pair_cap = 2 * tokens // owner_count
    destination = owners[:, 0]
    owner_iota = jnp.arange(owner_count, dtype=jnp.int32)
    my_destination = lax.dynamic_slice_in_dim(destination, seq_index * tokens, tokens)
    earlier = token_at[None, :] < token_at[:, None]
    local_rank = jnp.sum(((my_destination[:, None] == my_destination[None, :]) & earlier).astype(jnp.int32), axis=1)
    send_index = my_destination * pair_cap + local_rank
    from_each = jnp.sum((destination.reshape(owner_count, tokens) == seq_index).astype(jnp.int32), axis=1)
    lower = owner_iota[None, :] < owner_iota[:, None]
    offsets = jnp.sum(jnp.where(lower, from_each[None, :], 0), axis=1)
    pair_rank = jnp.arange(pair_cap, dtype=jnp.int32)
    slot_count = text_embed.shape[0]
    placement = jnp.where(
        pair_rank[None, :] < from_each[:, None], offsets[:, None] + pair_rank[None, :], slot_count
    ).reshape(-1)
    slot_at = jnp.arange(slot_count, dtype=jnp.int32)
    is_vision = slot_at < jnp.sum(from_each)


    outgoing, own_outgoing = language_rows(pos, merged_blocks, lang_gain, projections, send_index[None, :])
    l_width = text_embed.shape[1]
    out_cols = after(l_out, outgoing)
    other_out = [
        swap_cores(lax.dynamic_slice_in_dim(out_cols, (2 * ((z + d) % 4) + 1 - c) * l_width, l_width, 1))
        for d in range(4)
    ]

    def route(rows):
        arrived = lax.all_to_all(
            rows.reshape(owner_count, pair_cap, -1), seq, split_axis=0, concat_axis=0, tiled=True
        )
        return arrived.reshape(owner_count * pair_cap, -1)

    incoming, own_incoming = route(outgoing), route(own_outgoing)
    visual = is_vision.astype(jnp.int32)[:, None]
    lang_attended = pl.pallas_call(
        language_kernel,
        out_shape=jax.ShapeDtypeStruct((slot_count, l_query.shape[1]), BF),
        compiler_params=limit(16),
        name="language_kernel",
    )(incoming, text_qkv, placement[None, :], visual, segment_ids[:, None], segment_ids[None, :])
    filled = pl.pallas_call(
        fill_kernel,
        out_shape=jax.ShapeDtypeStruct(text_embed.shape, BF),
        compiler_params=limit(16),
        name="fill_kernel",
    )(own_incoming, text_embed, placement[None, :], visual)

    theirs = swap_cores(lang_attended)

    def block(d, count):
        return column_block(lang_attended, theirs, l_out, other_out[d], 2 * ((z + d) % 4) + c, count)

    far, after_one, before_one, own = block(2, 2), block(1, 2), block(3, 2), block(0, 1)
    up, down = shift(far[0], "z", 1), shift(far[1], "z", -1)
    nxt_high, prv_low = shift(after_one[1], "z", 1), shift(before_one[0], "z", -1)
    nxt_low = shift((after_one[0].astype(F32) + up.astype(F32)).astype(BF), "z", 1)
    prv_high = shift((before_one[1].astype(F32) + down.astype(F32)).astype(BF), "z", -1)
    total = jnp.concatenate(
        [nxt_low.astype(F32) + prv_low.astype(F32), nxt_high.astype(F32) + prv_high.astype(F32)], axis=0
    )
    return (filled.astype(F32) + own[0].astype(F32) + total).astype(BF)


def solution(mesh):
    fine = Mesh(mesh.devices.reshape(4, 4, 4, 2), ("x", "y", "z", "c"))
    seq, tp = ("x", "y"), ("z", "c")
    in_specs = (
        P(seq, None), P(), P(), P(None, tp), P(None, tp), P(None, tp), P(tp, None), P(), P(seq, tp), P(tp, seq),
        P(), P(seq, tp), P(seq), P(), P(None, tp), P(None, tp), P(None, tp), P(tp, None),
    )


    return jax.shard_map(body, mesh=fine, in_specs=in_specs, out_specs=P(seq, tp), check_vma=False)
```

```python
import math

import jax
import jax.numpy as jnp
from jax import lax
from jax.experimental import pallas as pl
from jax.experimental.pallas import tpu as pltpu
from jax.sharding import Mesh
from jax.sharding import PartitionSpec as P

DV = 1280
VHEADS = 16
D = 8192
LHD = 128
HEAD = DV // VHEADS
EPSILON = 1e-06
NEG_FILL = -1e30
BF = jnp.bfloat16
F32 = jnp.float32


def shift(value, axis, step):
    count = lax.axis_size(axis)
    return lax.ppermute(value, axis, [(i, (i + step) % count) for i in range(count)])


def after(value, other):
    return lax.optimization_barrier((value, other))[0]


def limit(mebibytes):
    return pltpu.CompilerParams(vmem_limit_bytes=mebibytes << 20)


def gather_direct(value, axis):
    return [value] + [shift(value, axis, d) for d in (1, 2, 3)]


def gather_halves(value, axis):
    return [value, shift(value, axis, 1), shift(value, axis, -1)]


def far_halves(parts, axis, held):
    half = parts[0].shape[0] // 2
    before, behind = after(parts[1], held), after(parts[2], held)
    low, high = shift(before[:half], axis, 1), shift(behind[half:], axis, -1)
    return parts + [low, high]


def swap_cores(value):
    return shift(value, "c", 1)


def reduce_direct(blocks, axis):
    total = blocks[0].astype(F32)
    for d in (1, 2, 3):
        total = total + shift(blocks[d], axis, d).astype(F32)
    return total


def rms_scaled(values, norm_gain):
    mean_square = jnp.mean(values * values, axis=-1, keepdims=True)
    return (values * lax.rsqrt(mean_square + EPSILON) * norm_gain).astype(BF)


def project_kernel(pos_ref, x_ref, gain_ref, wq_ref, wk_ref, wv_ref, down_ref, kv_ref, q_ref, *rest):
    normed = rms_scaled(x_ref[...].astype(F32), gain_ref[...][None, :])
    width = wq_ref.shape[0]

    def project(weight):
        return lax.dot_general(weight, normed, (((1,), (1,)), ((), ())), preferred_element_type=F32).astype(BF)

    kv_ref[:width] = project(wk_ref[...])
    kv_ref[width:] = project(wv_ref[...])
    q_ref[...] = project(wq_ref[...])
    picked, quarters = rest[:4], rest[4:]
    narrow = quarters[0].shape[1]
    for e in range(4):
        start = pl.multiple_of((pos_ref[2] + e) % 4 * narrow, narrow)
        quarters[e][...] = down_ref[:, pl.ds(start, narrow)]
    count = x_ref.shape[0]
    for d in range(4):
        tokens = picked[d].shape[0]
        token = lax.broadcasted_iota(jnp.int32, (tokens, count), 0) + (pos_ref[3] * tokens if d else 0)
        patch = lax.broadcasted_iota(jnp.int32, (tokens, count), 1)
        pick = (patch == 4 * token + (pos_ref[0] + d) % 4).astype(F32).astype(BF)
        picked[d][...] = jnp.dot(pick, x_ref[...], preferred_element_type=F32).astype(BF)


def vision_kernel(pos_ref, q_ref, own_ref, left_ref, right_ref, id_ref, *refs):
    outs, (queries_s, keys_s, values_s, mixed_s) = refs[:4], refs[4:]
    rows, count = q_ref.shape
    tokens, wide = count // 4, count // 2
    column = lax.broadcasted_iota(jnp.int32, (count, count), 1)
    source = lax.broadcasted_iota(jnp.int32, (count, count), 0)
    wanted = 4 * (column % tokens) + (column // tokens + pos_ref[0]) % 4
    order = (source == wanted).astype(F32).astype(BF)
    queries = jnp.dot(q_ref[...], order, preferred_element_type=F32).astype(BF)
    for part in range(2):
        queries_s[part] = queries[:, part * wide : (part + 1) * wide]
    for i, ref in enumerate((own_ref, left_ref, right_ref)):
        keys_s[:, i * count : (i + 1) * count] = ref[:rows]
        values_s[:, i * count : (i + 1) * count] = ref[rows:]
    patch = lax.broadcasted_iota(jnp.int32, (count, tokens), 0)
    token = lax.broadcasted_iota(jnp.int32, (count, tokens), 1)
    owner = (patch // 4 == token).astype(F32).astype(BF)
    ids = id_ref[...].astype(F32)
    key_ids = [
        lax.dot_general(
            owner, jnp.broadcast_to(ids[:, i * tokens : (i + 1) * tokens], (8, tokens)).astype(BF),
            (((1,), (1,)), ((), ())), preferred_element_type=F32,
        )[:, :1]
        for i in (1, 0, 2)
    ]
    own_ids = ids[:, tokens : 2 * tokens]
    allowed = jnp.concatenate(key_ids, axis=0) == jnp.concatenate([own_ids, own_ids], axis=1)
    scale = 1.0 / math.sqrt(HEAD)

    def one(step, _):
        lower = pl.multiple_of(step // 2 * HEAD, HEAD)
        scores = lax.dot_general(
            keys_s[pl.ds(lower, HEAD)], queries_s[step % 2, pl.ds(lower, HEAD)],
            (((0,), (0,)), ((), ())), preferred_element_type=F32,
        )
        scores = jnp.where(allowed, scores * scale, NEG_FILL)
        highest = jnp.max(scores, axis=0, keepdims=True)
        weights = jnp.where(allowed, jnp.exp(scores - highest), 0.0)
        totals = jnp.sum(weights, axis=0, keepdims=True)
        mixed = jnp.dot(values_s[pl.ds(lower, HEAD)], weights.astype(BF), preferred_element_type=F32)
        mixed_s[step % 2, pl.ds(lower, HEAD)] = (mixed / totals).astype(BF)
        return 0

    lax.fori_loop(0, 2 * (rows // HEAD), one, 0)
    for i in range(4):
        outs[i][...] = mixed_s[i // 2, :, i % 2 * tokens : (i % 2 + 1) * tokens]


def merge_kernel(pos_ref, *refs):
    att, weights, rest, (gain_ref, *ups), outs, (att_s, w_s, up_s, t_s, rest_s) = (
        refs[:8], refs[8:16], refs[16:23], refs[23:29], refs[29:33], refs[33:]
    )
    part, tokens = att[0].shape[0], rest[0].shape[0]
    half = tokens // 2
    for i in range(8):
        att_s[i * part : (i + 1) * part] = att[i][...]
    for r in range(4):
        for other in range(2):
            start = (2 * r + other) * part
            w_s[start : start + part] = weights[2 * r + other][...]
    rows = ups[0].shape[0]
    for d, offset, ref in ((0, 0, ups[0]), (1, 0, ups[1]), (3, 0, ups[2]), (2, 0, ups[3]), (2, rows // 2, ups[4])):
        start = pl.multiple_of((pos_ref[1] + 4 - d) % 4 * rows + offset, rows // 2)
        up_s[pl.ds(start, ref.shape[0])] = ref[...]
    rest_s[:tokens] = rest[0][...]
    for d in range(1, 4):
        for other in range(2):
            start = pl.multiple_of(d * tokens + (pos_ref[3] + other) % 2 * half, half)
            rest_s[pl.ds(start, half)] = rest[2 * d - 1 + other][...]
    state = lax.dot_general(att_s[...], w_s[...], (((0,), (0,)), ((), ())), preferred_element_type=F32)
    state = state + rest_s[...].astype(F32)
    normed = rms_scaled(state, gain_ref[...][None, :])
    t_s[...] = jnp.dot(normed, up_s[...], preferred_element_type=F32).T.astype(BF)
    for e in range(4):
        start = pl.multiple_of((pos_ref[0] + e) % 4 * part, part)
        term = t_s[pl.ds(start, part)]
        for d in range(4):
            g = (d + e) % 4
            outs[e][:, g * tokens : (g + 1) * tokens] = term[:, d * tokens : (d + 1) * tokens]


def regroup_kernel(pos_ref, *refs):
    blocks, outs = refs[:4], refs[4:]
    part = blocks[0].shape[0] // 4
    for e in range(4):
        start = pl.multiple_of((pos_ref[0] + e) % 4 * part, part)
        for r in range(4):
            outs[e][r * part : (r + 1) * part] = blocks[r][pl.ds(start, part)]


def down_kernel(pos_ref, *refs):
    hidden, parts, outs, (h_s, w_s) = refs[:8], refs[8:18], refs[18:22], refs[22:]
    x, y, c = pos_ref[0], pos_ref[1], pos_ref[3]
    part, tokens = hidden[0].shape[0], outs[0].shape[0]
    narrow = parts[0].shape[2]
    for i in range(8):
        h_s[i * part : (i + 1) * part] = hidden[i][...]

    def place(ref, other, d, first):
        for q in range(ref.shape[0]):
            at = (x + 4 - first - q) % 4 * 2 + (y + 4 - d) % 4 // 2
            column = pl.ds(pl.multiple_of(at * narrow, narrow), narrow)
            for r in range(4):
                start = (2 * r + other) * part
                w_s[start : start + part, column] = ref[q, r * part : (r + 1) * part]

    @pl.when((y + c) % 2 == 0)
    def _():
        for other in range(2):
            place(parts[5 * other], other, 0, 0)
            place(parts[5 * other + 3], other, 2, 0)
            place(parts[5 * other + 4], other, 2, 2)

    @pl.when((y + c) % 2 == 1)
    def _():
        for other in range(2):
            place(parts[5 * other + 1], other, 1, 0)
            place(parts[5 * other + 2], other, 3, 0)

    both = lax.dot_general(h_s[...], w_s[...], (((0,), (0,)), ((), ())), preferred_element_type=F32).astype(BF)
    for g in range(4):
        outs[(4 - g) % 4][...] = both[g * tokens : (g + 1) * tokens]


def rows_kernel(pos_ref, *refs, routed):
    count = 8 if routed else 10
    blocks, (gain_ref, *weights), rest = refs[:count], refs[count : count + 4], refs[count + 4 :]
    (send_ref, out_ref, own_ref, s, *buffers, sems) = rest if routed else (None, rest[0], None, rest[1], None)
    rows, width = s.shape[0], s.shape[1] // 8
    z, c = pos_ref[2], pos_ref[3]

    def copies(i):
        return [
            pltpu.make_async_copy(w.at[pl.ds(i * width, width)], b.at[pl.ds(i * width, width)], sems.at[i, j])
            for j, (w, b) in enumerate(zip(weights, buffers))
        ]

    copies_of = [copies(i) for i in range(8)] if routed else []
    for group in copies_of:
        for copy in group:
            copy.start()
    total = jnp.zeros((rows, 1), F32)
    if routed:
        narrow = width // 8
        for i in range(8):
            value = blocks[i][...].astype(F32)
            total = total + jnp.sum(value * value, axis=-1, keepdims=True)
            core = (c + i % 2) % 2
            for k in range(8):
                start = pl.multiple_of((core + 2 * k) * 4 * narrow + (z + 4 - i // 2) % 4 * narrow, narrow)
                s[:, pl.ds(start, narrow)] = blocks[i][:, k * narrow : (k + 1) * narrow]
    else:
        half = rows // 2
        for other in range(2):
            own, before, behind, low, high = blocks[5 * other : 5 * other + 5]
            for r, first, ref in ((0, 0, own), (1, 0, before), (3, 0, behind), (2, 0, low), (2, half, high)):
                start = pl.multiple_of((2 * ((z + 4 - r) % 4) + (c + other) % 2) * width, width)
                s[first : first + ref.shape[0], pl.ds(start, width)] = ref[...]
        for i in range(8):
            value = s[:, i * width : (i + 1) * width].astype(F32)
            total = total + jnp.sum(value * value, axis=-1, keepdims=True)
    scale = lax.rsqrt(total / D + EPSILON)

    def one(i, sums):
        start = i * width if isinstance(i, int) else pl.multiple_of(i * width, width)
        columns = pl.ds(start, width)
        normed = (s[:, columns].astype(F32) * scale * gain_ref[:, columns]).astype(BF)
        return tuple(t + jnp.dot(normed, w[columns], preferred_element_type=F32) for t, w in zip(sums, weights))

    sums = tuple(jnp.zeros((rows, w.shape[1]), F32) for w in weights)
    if routed:
        weights = buffers
        for i in range(8):
            for copy in copies_of[i]:
                copy.wait()
            sums = one(i, sums)
    else:
        sums = lax.fori_loop(0, 8, one, sums)
    whole = jnp.concatenate(sums, axis=1).astype(BF)
    if routed:
        pick = (lax.broadcasted_iota(jnp.int32, (out_ref.shape[0], rows), 0) == send_ref[...]).astype(F32).astype(BF)
        out_ref[...] = jnp.dot(pick, whole, preferred_element_type=F32).astype(BF)
        own = s[:, pl.ds(pl.multiple_of((2 * z + c) * width, width), width)]
        own_ref[...] = jnp.dot(pick, own, preferred_element_type=F32).astype(BF)
    else:
        out_ref[...] = whole


def language_rows(pos, blocks, gain, weights, send=None):
    rows, width = blocks[0].shape
    total = sum(w.shape[1] for w in weights)
    operands = [pos, *blocks, gain[None, :], *weights]
    vmem = pl.BlockSpec(memory_space=pltpu.VMEM)
    where = vmem if send is None else pl.BlockSpec(memory_space=pltpu.HBM)
    specs = [pl.BlockSpec(memory_space=pltpu.SMEM)] + [vmem] * (len(blocks) + 1) + [where] * 3
    scratch = [pltpu.VMEM((rows, 8 * width), BF)]
    shapes = [jax.ShapeDtypeStruct((rows, total), BF)]
    if send is not None:
        operands.append(send)
        specs.append(vmem)
        scratch += [pltpu.VMEM(w.shape, BF) for w in weights] + [pltpu.SemaphoreType.DMA((8, 3))]
        shapes = [jax.ShapeDtypeStruct((2 * rows, n), BF) for n in (total, width)]
    return pl.pallas_call(
        lambda *refs: rows_kernel(*refs, routed=send is not None),
        in_specs=specs,
        out_specs=[vmem] * len(shapes),
        out_shape=shapes,
        scratch_shapes=scratch,
        compiler_params=limit(32 if send is None else 60),
        name="rows_kernel",
    )(*operands)


def fill_kernel(in_ref, embed_ref, place_ref, vis_ref, out_ref):
    slots = embed_ref.shape[0]
    spread = (lax.broadcasted_iota(jnp.int32, (slots, slots), 0) == place_ref[...]).astype(F32).astype(BF)
    placed = jnp.dot(spread, in_ref[...], preferred_element_type=F32)
    out_ref[...] = jnp.where(vis_ref[...] > 0, placed, embed_ref[...].astype(F32)).astype(BF)


def language_kernel(in_ref, text_ref, place_ref, vis_ref, sega_ref, segb_ref, out_ref):
    slots = text_ref.shape[0]
    row = lax.broadcasted_iota(jnp.int32, (slots, slots), 0)
    col = lax.broadcasted_iota(jnp.int32, (slots, slots), 1)
    spread = (row == place_ref[...]).astype(F32).astype(BF)
    visual = vis_ref[...] > 0
    placed = jnp.dot(spread, in_ref[...], preferred_element_type=F32)
    qkv = jnp.where(visual, placed, text_ref[...].astype(F32)).astype(BF)
    allowed = (sega_ref[...] == segb_ref[...]) & (col <= row)
    width = out_ref.shape[1]
    keys, values = qkv[:, width : width + LHD], qkv[:, width + LHD :]
    for head in range(width // LHD):
        scores = lax.dot_general(
            qkv[:, head * LHD : (head + 1) * LHD], keys, (((1,), (1,)), ((), ())), preferred_element_type=F32
        ) * (1.0 / math.sqrt(LHD))
        scores = jnp.where(allowed, scores, NEG_FILL)
        highest = jnp.max(scores, axis=-1, keepdims=True)
        weights = jnp.where(allowed, jnp.exp(scores - highest), 0.0)
        totals = jnp.sum(weights, axis=-1, keepdims=True)
        mixed = jnp.dot(weights.astype(BF), values, preferred_element_type=F32)
        out_ref[:, head * LHD : (head + 1) * LHD] = (mixed / totals).astype(BF)


def columns_kernel(pos_ref, source_ref, mine_ref, theirs_ref, sems):
    width = mine_ref.shape[2]
    copies = []
    for d in range(4):
        for i, (ref, core) in enumerate(((mine_ref, pos_ref[3]), (theirs_ref, 1 - pos_ref[3]))):
            start = pl.multiple_of((2 * ((pos_ref[2] + d) % 4) + core) * width, width)
            copies.append(pltpu.make_async_copy(source_ref.at[:, pl.ds(start, width)], ref.at[d], sems.at[d, i]))
    for copy in copies:
        copy.start()
    for copy in copies:
        copy.wait()


def block_kernel(mine_ref, theirs_ref, right_ref, other_ref, *outs):
    both = jnp.dot(theirs_ref[...], other_ref[0], preferred_element_type=F32) + jnp.dot(
        mine_ref[...], right_ref[0], preferred_element_type=F32
    )
    rows = outs[0].shape[0]
    for i, out in enumerate(outs):
        out[...] = both[i * rows : (i + 1) * rows].astype(BF)


def column_block(mine, theirs, right, other, d, count):
    depth, width = right.shape[1:]
    rows = mine.shape[0] // count
    whole = lambda shape: pl.BlockSpec(shape, lambda i: (0, 0))
    block = pl.BlockSpec((1, depth, width), lambda i: (d, 0, 0))
    return pl.pallas_call(
        block_kernel,
        grid=(1,),
        in_specs=[whole(mine.shape), whole(mine.shape), block, block],
        out_specs=[whole((rows, width))] * count,
        out_shape=[jax.ShapeDtypeStruct((rows, width), BF)] * count,
        compiler_params=limit(16),
        name="block_kernel",
    )(mine, theirs, right, other)


def body(
    patches, image_ids, vision_gain, v_query, v_key, v_value, v_out, merge_gain, merge_up, merge_down,
    owners, text_embed, segment_ids, lang_gain, l_query, l_key, l_value, l_out,
):
    x, y, z, c = (lax.axis_index(a) for a in ("x", "y", "z", "c"))
    seq_index = 4 * x + y
    row_count = patches.shape[0]
    tokens = row_count // 4
    local = v_query.shape[1]

    pos = jnp.stack([x, y, z, c]).astype(jnp.int32)
    scalars = pl.BlockSpec(memory_space=pltpu.SMEM)
    vmem = pl.BlockSpec(memory_space=pltpu.VMEM)

    key_value, query_own, *cut = pl.pallas_call(
        project_kernel,
        in_specs=[scalars] + [vmem] * 6,
        out_specs=[vmem] * 10,
        out_shape=[
            jax.ShapeDtypeStruct((2 * local, row_count), BF),
            jax.ShapeDtypeStruct((local, row_count), BF),
        ]
        + [jax.ShapeDtypeStruct((tokens, DV), BF)]
        + [jax.ShapeDtypeStruct((tokens // 2, DV), BF)] * 3
        + [jax.ShapeDtypeStruct((merge_down.shape[0], merge_down.shape[1] // 4), BF)] * 4,
        name="project_kernel",
    )(pos, patches, vision_gain, v_query.T, v_key.T, v_value.T, merge_down)
    picked, quarters = cut[:4], cut[4:]
    seq = ("x", "y")
    left, right = shift(key_value, seq, 1), shift(key_value, seq, -1)
    padded_ids = jnp.pad(image_ids, (tokens, tokens), constant_values=-1)
    near_ids = lax.dynamic_slice_in_dim(padded_ids, seq_index * tokens, 3 * tokens)
    attended = pl.pallas_call(
        vision_kernel,
        in_specs=[scalars] + [vmem] * 5,
        out_specs=[vmem] * 4,
        out_shape=[jax.ShapeDtypeStruct((local, tokens), BF)] * 4,
        scratch_shapes=[
            pltpu.VMEM((2, local, row_count // 2), BF),
            pltpu.VMEM((local, 3 * row_count), BF),
            pltpu.VMEM((local, 3 * row_count), BF),
            pltpu.VMEM((2, local, row_count // 2), BF),
        ],
        compiler_params=limit(24),
        name="vision_kernel",
    )(
        pos, query_own, key_value, left, right, near_ids[None, :]
    )

    token_at = jnp.arange(tokens, dtype=jnp.int32)
    down_z = [quarters[0]] + [shift(quarters[e], "z", e) for e in (1, 2, 3)]
    out_parts = gather_direct(after(v_out, query_own), "z")

    att_moved = [attended[0]] + [shift(attended[d], "x", d) for d in (1, 2, 3)]
    up_parts = gather_halves(after(merge_up, attended[0]), "y")
    att_rows = jnp.concatenate(att_moved, axis=1)
    att_z = gather_direct(att_rows, "z")
    up_parts = far_halves(up_parts, "y", att_rows)
    moved_patches = [shift(after(picked[d], att_rows), "x", d) for d in (1, 2, 3)]
    residual = [picked[0]] + [v for p in moved_patches for v in (p, swap_cores(p))]
    text_parts = gather_halves(after(after(text_embed, att_z[2]), att_z[1]), "z")
    att_all = [v for block in att_z for v in (block, swap_cores(block))]
    out_all = [v for part in out_parts for v in (part, swap_cores(after(part, att_rows)))]
    down_terms = pl.pallas_call(
        regroup_kernel,
        in_specs=[scalars] + [vmem] * 4,
        out_specs=[vmem] * 4,
        out_shape=[jax.ShapeDtypeStruct(quarters[0].shape, BF)] * 4,
        compiler_params=limit(8),
        name="regroup_kernel",
    )(pos, *[after(part, attended[0]) for part in down_z])
    down_own = [down_terms[0]] + [shift(down_terms[e], "x", e) for e in (1, 2, 3)]
    down_parts = gather_halves(jnp.stack([after(part, att_rows) for part in down_own]), "y")
    up_terms = pl.pallas_call(
        merge_kernel,
        in_specs=[scalars] + [vmem] * 29,
        out_specs=[vmem] * 4,
        out_shape=[jax.ShapeDtypeStruct((local, row_count), BF)] * 4,
        scratch_shapes=[
            pltpu.VMEM((8 * local, row_count), BF),
            pltpu.VMEM((8 * local, DV), BF),
            pltpu.VMEM((4 * merge_up.shape[0], merge_up.shape[1]), BF),
            pltpu.VMEM((4 * local, row_count), BF),
            pltpu.VMEM((row_count, DV), BF),
        ],
        compiler_params=limit(32),
        name="merge_kernel",
    )(pos, *att_all, *out_all, *residual, merge_gain, *up_parts)
    hidden_sum = reduce_direct(up_terms, "x")
    hidden = jax.nn.gelu(hidden_sum, approximate=False).astype(BF)
    down_parts = far_halves(down_parts, "y", up_terms[0])
    hidden_z = gather_direct(hidden, "z")
    hidden_all = [v for block in hidden_z for v in (block, swap_cores(block))]
    text_parts = far_halves(text_parts, "z", hidden)
    down_all = down_parts + [swap_cores(part) for part in down_parts]
    down_terms = pl.pallas_call(
        down_kernel,
        in_specs=[scalars] + [vmem] * 18,
        out_specs=[vmem] * 4,
        out_shape=[jax.ShapeDtypeStruct((tokens, 2 * merge_down.shape[1]), BF)] * 4,
        scratch_shapes=[pltpu.VMEM((8 * local, row_count), BF), pltpu.VMEM((8 * local, 2 * merge_down.shape[1]), BF)],
        compiler_params=limit(24),
        name="down_kernel",
    )(pos, *hidden_all, *down_all)
    merged = reduce_direct(down_terms, "x").astype(BF)
    merged_z = gather_direct(merged, "z")
    merged_blocks = [v for block in merged_z for v in (block, swap_cores(block))]
    text_all = text_parts + [swap_cores(after(part, hidden)) for part in text_parts]
    projections = (l_query, l_key, l_value)
    (text_qkv,) = language_rows(pos, text_all, lang_gain, projections)

    owner_count = 16
    pair_cap = 2 * tokens // owner_count
    destination = owners[:, 0]
    owner_iota = jnp.arange(owner_count, dtype=jnp.int32)
    my_destination = lax.dynamic_slice_in_dim(destination, seq_index * tokens, tokens)
    earlier = token_at[None, :] < token_at[:, None]
    local_rank = jnp.sum(((my_destination[:, None] == my_destination[None, :]) & earlier).astype(jnp.int32), axis=1)
    send_index = my_destination * pair_cap + local_rank
    from_each = jnp.sum((destination.reshape(owner_count, tokens) == seq_index).astype(jnp.int32), axis=1)
    lower = owner_iota[None, :] < owner_iota[:, None]
    offsets = jnp.sum(jnp.where(lower, from_each[None, :], 0), axis=1)
    pair_rank = jnp.arange(pair_cap, dtype=jnp.int32)
    slot_count = text_embed.shape[0]
    placement = jnp.where(
        pair_rank[None, :] < from_each[:, None], offsets[:, None] + pair_rank[None, :], slot_count
    ).reshape(-1)
    slot_at = jnp.arange(slot_count, dtype=jnp.int32)
    is_vision = slot_at < jnp.sum(from_each)


    outgoing, own_outgoing = language_rows(pos, merged_blocks, lang_gain, projections, send_index[None, :])
    l_width = text_embed.shape[1]
    own_out, their_out = pl.pallas_call(
        columns_kernel,
        in_specs=[scalars, pl.BlockSpec(memory_space=pltpu.HBM)],
        out_specs=[vmem] * 2,
        out_shape=[jax.ShapeDtypeStruct((4, l_out.shape[0], l_width), BF)] * 2,
        scratch_shapes=[pltpu.SemaphoreType.DMA((4, 2))],
        compiler_params=limit(16),
        name="columns_kernel",
    )(pos, after(l_out, merged))
    other_out = swap_cores(their_out)

    def route(rows):
        arrived = lax.all_to_all(
            rows.reshape(owner_count, pair_cap, -1), seq, split_axis=0, concat_axis=0, tiled=True
        )
        return arrived.reshape(owner_count * pair_cap, -1)

    incoming = route(outgoing)
    own_incoming = route(own_outgoing)
    visual = is_vision.astype(jnp.int32)[:, None]
    lang_attended = pl.pallas_call(
        language_kernel,
        out_shape=jax.ShapeDtypeStruct((slot_count, l_query.shape[1]), BF),
        compiler_params=limit(16),
        name="language_kernel",
    )(incoming, text_qkv, placement[None, :], visual, segment_ids[:, None], segment_ids[None, :])
    filled = pl.pallas_call(
        fill_kernel,
        out_shape=jax.ShapeDtypeStruct(text_embed.shape, BF),
        compiler_params=limit(16),
        name="fill_kernel",
    )(own_incoming, text_embed, placement[None, :], visual)

    theirs = swap_cores(lang_attended)

    def block(d, count):
        return column_block(lang_attended, theirs, own_out, other_out, d, count)

    far, after_one, before_one, own = block(2, 2), block(1, 2), block(3, 2), block(0, 1)
    up, down = shift(far[0], "z", 1), shift(far[1], "z", -1)
    nxt_high, prv_low = shift(after_one[1], "z", 1), shift(before_one[0], "z", -1)
    nxt_low = shift((after_one[0].astype(F32) + up.astype(F32)).astype(BF), "z", 1)
    prv_high = shift((before_one[1].astype(F32) + down.astype(F32)).astype(BF), "z", -1)
    total = jnp.concatenate(
        [nxt_low.astype(F32) + prv_low.astype(F32), nxt_high.astype(F32) + prv_high.astype(F32)], axis=0
    )
    return (filled.astype(F32) + own[0].astype(F32) + total).astype(BF)


def solution(mesh):
    fine = Mesh(mesh.devices.reshape(4, 4, 4, 2), ("x", "y", "z", "c"))
    seq, tp = ("x", "y"), ("z", "c")
    in_specs = (
        P(seq, None), P(), P(), P(None, tp), P(None, tp), P(None, tp), P(tp, None), P(), P(seq, tp), P(tp, seq),
        P(), P(seq, tp), P(seq), P(), P(None, tp), P(None, tp), P(None, tp), P(tp, None),
    )


    return jax.shard_map(body, mesh=fine, in_specs=in_specs, out_specs=P(seq, tp), check_vma=False)
```

```python
import math

import jax
import jax.numpy as jnp
from jax import lax
from jax.experimental import pallas as pl
from jax.experimental.pallas import tpu as pltpu
from jax.sharding import Mesh
from jax.sharding import PartitionSpec as P

DV = 1280
VHEADS = 16
D = 8192
LHD = 128
HEAD = DV // VHEADS
EPSILON = 1e-06
NEG_FILL = -1e30
BF = jnp.bfloat16
F32 = jnp.float32


def shift(value, axis, step):
    count = lax.axis_size(axis)
    return lax.ppermute(value, axis, [(i, (i + step) % count) for i in range(count)])


def after(value, other):
    return lax.optimization_barrier((value, other))[0]


def limit(mebibytes):
    return pltpu.CompilerParams(vmem_limit_bytes=mebibytes << 20)


def gather_direct(value, axis):
    return [value] + [shift(value, axis, d) for d in (1, 2, 3)]


def gather_halves(value, axis):
    return [value, shift(value, axis, 1), shift(value, axis, -1)]


def far_halves(parts, axis, held):
    half = parts[0].shape[0] // 2
    before, behind = after(parts[1], held), after(parts[2], held)
    low, high = shift(before[:half], axis, 1), shift(behind[half:], axis, -1)
    return parts + [low, high]


def swap_cores(value):
    return shift(value, "c", 1)


def reduce_direct(blocks, axis):
    total = blocks[0].astype(F32)
    for d in (1, 2, 3):
        total = total + shift(blocks[d], axis, d).astype(F32)
    return total


def rms_scaled(values, norm_gain):
    mean_square = jnp.mean(values * values, axis=-1, keepdims=True)
    return (values * lax.rsqrt(mean_square + EPSILON) * norm_gain).astype(BF)


def project_kernel(pos_ref, x_ref, gain_ref, wq_ref, wk_ref, wv_ref, down_ref, kv_ref, q_ref, *rest):
    normed = rms_scaled(x_ref[...].astype(F32), gain_ref[...][None, :])
    width = wq_ref.shape[0]

    def project(weight):
        return lax.dot_general(weight, normed, (((1,), (1,)), ((), ())), preferred_element_type=F32).astype(BF)

    kv_ref[:width] = project(wk_ref[...])
    kv_ref[width:] = project(wv_ref[...])
    q_ref[...] = project(wq_ref[...])
    picked, quarters = rest[:4], rest[4:]
    narrow = quarters[0].shape[1]
    for e in range(4):
        start = pl.multiple_of((pos_ref[2] + e) % 4 * narrow, narrow)
        quarters[e][...] = down_ref[:, pl.ds(start, narrow)]
    count = x_ref.shape[0]
    for d in range(4):
        tokens = picked[d].shape[0]
        token = lax.broadcasted_iota(jnp.int32, (tokens, count), 0) + (pos_ref[3] * tokens if d else 0)
        patch = lax.broadcasted_iota(jnp.int32, (tokens, count), 1)
        pick = (patch == 4 * token + (pos_ref[0] + d) % 4).astype(F32).astype(BF)
        picked[d][...] = jnp.dot(pick, x_ref[...], preferred_element_type=F32).astype(BF)


def vision_kernel(pos_ref, q_ref, own_ref, left_ref, right_ref, id_ref, *refs):
    outs, (queries_s, keys_s, values_s, mixed_s) = refs[:4], refs[4:]
    rows, count = q_ref.shape
    tokens, wide = count // 4, count // 2
    column = lax.broadcasted_iota(jnp.int32, (count, count), 1)
    source = lax.broadcasted_iota(jnp.int32, (count, count), 0)
    wanted = 4 * (column % tokens) + (column // tokens + pos_ref[0]) % 4
    order = (source == wanted).astype(F32).astype(BF)
    queries = jnp.dot(q_ref[...], order, preferred_element_type=F32).astype(BF)
    for part in range(2):
        queries_s[part] = queries[:, part * wide : (part + 1) * wide]
    for i, ref in enumerate((own_ref, left_ref, right_ref)):
        keys_s[:, i * count : (i + 1) * count] = ref[:rows]
        values_s[:, i * count : (i + 1) * count] = ref[rows:]
    patch = lax.broadcasted_iota(jnp.int32, (count, tokens), 0)
    token = lax.broadcasted_iota(jnp.int32, (count, tokens), 1)
    owner = (patch // 4 == token).astype(F32).astype(BF)
    ids = id_ref[...].astype(F32)
    key_ids = [
        lax.dot_general(
            owner, jnp.broadcast_to(ids[:, i * tokens : (i + 1) * tokens], (8, tokens)).astype(BF),
            (((1,), (1,)), ((), ())), preferred_element_type=F32,
        )[:, :1]
        for i in (1, 0, 2)
    ]
    own_ids = ids[:, tokens : 2 * tokens]
    allowed = jnp.concatenate(key_ids, axis=0) == jnp.concatenate([own_ids, own_ids], axis=1)
    scale = math.log2(math.e) / math.sqrt(HEAD)

    def one(step, _):
        lower = pl.multiple_of(step // 2 * HEAD, HEAD)
        scores = lax.dot_general(
            keys_s[pl.ds(lower, HEAD)], queries_s[step % 2, pl.ds(lower, HEAD)],
            (((0,), (0,)), ((), ())), preferred_element_type=F32,
        )
        scores = jnp.where(allowed, scores * scale, NEG_FILL)
        highest = jnp.max(scores, axis=0, keepdims=True)
        weights = jnp.exp2(scores - highest)
        totals = jnp.sum(weights, axis=0, keepdims=True)
        mixed = jnp.dot(values_s[pl.ds(lower, HEAD)], weights.astype(BF), preferred_element_type=F32)
        mixed_s[step % 2, pl.ds(lower, HEAD)] = (mixed / totals).astype(BF)
        return 0

    lax.fori_loop(0, 2 * (rows // HEAD), one, 0)
    for i in range(4):
        outs[i][...] = mixed_s[i // 2, :, i % 2 * tokens : (i % 2 + 1) * tokens]


def merge_kernel(pos_ref, *refs):
    att, weights, rest, (gain_ref, *ups), outs, (att_s, w_s, up_s, t_s, rest_s) = (
        refs[:8], refs[8:16], refs[16:23], refs[23:29], refs[29:33], refs[33:]
    )
    part, tokens = att[0].shape[0], rest[0].shape[0]
    half = tokens // 2
    for i in range(8):
        att_s[i * part : (i + 1) * part] = att[i][...]
    for r in range(4):
        for other in range(2):
            start = (2 * r + other) * part
            w_s[start : start + part] = weights[2 * r + other][...]
    rows = ups[0].shape[0]
    for d, offset, ref in ((0, 0, ups[0]), (1, 0, ups[1]), (3, 0, ups[2]), (2, 0, ups[3]), (2, rows // 2, ups[4])):
        start = pl.multiple_of((pos_ref[1] + 4 - d) % 4 * rows + offset, rows // 2)
        up_s[pl.ds(start, ref.shape[0])] = ref[...]
    rest_s[:tokens] = rest[0][...]
    for d in range(1, 4):
        for other in range(2):
            start = pl.multiple_of(d * tokens + (pos_ref[3] + other) % 2 * half, half)
            rest_s[pl.ds(start, half)] = rest[2 * d - 1 + other][...]
    state = lax.dot_general(att_s[...], w_s[...], (((0,), (0,)), ((), ())), preferred_element_type=F32)
    state = state + rest_s[...].astype(F32)
    normed = rms_scaled(state, gain_ref[...][None, :])
    t_s[...] = jnp.dot(normed, up_s[...], preferred_element_type=F32).T.astype(BF)
    for e in range(4):
        start = pl.multiple_of((pos_ref[0] + e) % 4 * part, part)
        term = t_s[pl.ds(start, part)]
        for d in range(4):
            g = (d + e) % 4
            outs[e][:, g * tokens : (g + 1) * tokens] = term[:, d * tokens : (d + 1) * tokens]


def regroup_kernel(pos_ref, *refs):
    blocks, outs = refs[:4], refs[4:]
    part = blocks[0].shape[0] // 4
    for e in range(4):
        start = pl.multiple_of((pos_ref[0] + e) % 4 * part, part)
        for r in range(4):
            outs[e][r * part : (r + 1) * part] = blocks[r][pl.ds(start, part)]


def down_kernel(pos_ref, *refs):
    hidden, parts, outs, (h_s, w_s) = refs[:8], refs[8:18], refs[18:22], refs[22:]
    x, y, c = pos_ref[0], pos_ref[1], pos_ref[3]
    part, tokens = hidden[0].shape[0], outs[0].shape[0]
    narrow = parts[0].shape[2]
    for i in range(8):
        h_s[i * part : (i + 1) * part] = hidden[i][...]

    def place(ref, other, d, first):
        for q in range(ref.shape[0]):
            at = (x + 4 - first - q) % 4 * 2 + (y + 4 - d) % 4 // 2
            column = pl.ds(pl.multiple_of(at * narrow, narrow), narrow)
            for r in range(4):
                start = (2 * r + other) * part
                w_s[start : start + part, column] = ref[q, r * part : (r + 1) * part]

    @pl.when((y + c) % 2 == 0)
    def _():
        for other in range(2):
            place(parts[5 * other], other, 0, 0)
            place(parts[5 * other + 3], other, 2, 0)
            place(parts[5 * other + 4], other, 2, 2)

    @pl.when((y + c) % 2 == 1)
    def _():
        for other in range(2):
            place(parts[5 * other + 1], other, 1, 0)
            place(parts[5 * other + 2], other, 3, 0)

    both = lax.dot_general(h_s[...], w_s[...], (((0,), (0,)), ((), ())), preferred_element_type=F32).astype(BF)
    for g in range(4):
        outs[(4 - g) % 4][...] = both[g * tokens : (g + 1) * tokens]


def rows_kernel(pos_ref, *refs, routed):
    count = 8 if routed else 10
    blocks, (gain_ref, *weights), rest = refs[:count], refs[count : count + 4], refs[count + 4 :]
    (send_ref, out_ref, own_ref, s, *buffers, sems) = rest if routed else (None, rest[0], None, rest[1], None)
    rows, width = s.shape[0], s.shape[1] // 8
    z, c = pos_ref[2], pos_ref[3]

    def copies(i):
        return [
            pltpu.make_async_copy(w.at[pl.ds(i * width, width)], b.at[pl.ds(i * width, width)], sems.at[i, j])
            for j, (w, b) in enumerate(zip(weights, buffers))
        ]

    copies_of = [copies(i) for i in range(8)] if routed else []
    for group in copies_of:
        for copy in group:
            copy.start()
    total = jnp.zeros((rows, 1), F32)
    if routed:
        narrow = width // 8
        for i in range(8):
            value = blocks[i][...].astype(F32)
            total = total + jnp.sum(value * value, axis=-1, keepdims=True)
            core = (c + i % 2) % 2
            for k in range(8):
                start = pl.multiple_of((core + 2 * k) * 4 * narrow + (z + 4 - i // 2) % 4 * narrow, narrow)
                s[:, pl.ds(start, narrow)] = blocks[i][:, k * narrow : (k + 1) * narrow]
    else:
        half = rows // 2
        for other in range(2):
            own, before, behind, low, high = blocks[5 * other : 5 * other + 5]
            for r, first, ref in ((0, 0, own), (1, 0, before), (3, 0, behind), (2, 0, low), (2, half, high)):
                start = pl.multiple_of((2 * ((z + 4 - r) % 4) + (c + other) % 2) * width, width)
                s[first : first + ref.shape[0], pl.ds(start, width)] = ref[...]
        for i in range(8):
            value = s[:, i * width : (i + 1) * width].astype(F32)
            total = total + jnp.sum(value * value, axis=-1, keepdims=True)
    scale = lax.rsqrt(total / D + EPSILON)

    def one(i, sums):
        start = i * width if isinstance(i, int) else pl.multiple_of(i * width, width)
        columns = pl.ds(start, width)
        normed = (s[:, columns].astype(F32) * scale * gain_ref[:, columns]).astype(BF)
        return tuple(t + jnp.dot(normed, w[columns], preferred_element_type=F32) for t, w in zip(sums, weights))

    sums = tuple(jnp.zeros((rows, w.shape[1]), F32) for w in weights)
    if routed:
        weights = buffers
        for i in range(8):
            for copy in copies_of[i]:
                copy.wait()
            sums = one(i, sums)
    else:
        sums = lax.fori_loop(0, 8, one, sums)
    whole = jnp.concatenate(sums, axis=1).astype(BF)
    if routed:
        pick = (lax.broadcasted_iota(jnp.int32, (out_ref.shape[0], rows), 0) == send_ref[...]).astype(F32).astype(BF)
        out_ref[...] = jnp.dot(pick, whole, preferred_element_type=F32).astype(BF)
        own = s[:, pl.ds(pl.multiple_of((2 * z + c) * width, width), width)]
        own_ref[...] = jnp.dot(pick, own, preferred_element_type=F32).astype(BF)
    else:
        out_ref[...] = whole


def language_rows(pos, blocks, gain, weights, send=None):
    rows, width = blocks[0].shape
    total = sum(w.shape[1] for w in weights)
    operands = [pos, *blocks, gain[None, :], *weights]
    vmem = pl.BlockSpec(memory_space=pltpu.VMEM)
    where = vmem if send is None else pl.BlockSpec(memory_space=pltpu.HBM)
    specs = [pl.BlockSpec(memory_space=pltpu.SMEM)] + [vmem] * (len(blocks) + 1) + [where] * 3
    scratch = [pltpu.VMEM((rows, 8 * width), BF)]
    shapes = [jax.ShapeDtypeStruct((rows, total), BF)]
    if send is not None:
        operands.append(send)
        specs.append(vmem)
        scratch += [pltpu.VMEM(w.shape, BF) for w in weights] + [pltpu.SemaphoreType.DMA((8, 3))]
        shapes = [jax.ShapeDtypeStruct((2 * rows, n), BF) for n in (total, width)]
    return pl.pallas_call(
        lambda *refs: rows_kernel(*refs, routed=send is not None),
        in_specs=specs,
        out_specs=[vmem] * len(shapes),
        out_shape=shapes,
        scratch_shapes=scratch,
        compiler_params=limit(32 if send is None else 60),
        name="rows_kernel",
    )(*operands)


def fill_kernel(in_ref, embed_ref, place_ref, vis_ref, out_ref):
    slots = embed_ref.shape[0]
    spread = (lax.broadcasted_iota(jnp.int32, (slots, slots), 0) == place_ref[...]).astype(F32).astype(BF)
    placed = jnp.dot(spread, in_ref[...], preferred_element_type=F32)
    out_ref[...] = jnp.where(vis_ref[...] > 0, placed, embed_ref[...].astype(F32)).astype(BF)


def language_kernel(in_ref, text_ref, place_ref, vis_ref, sega_ref, segb_ref, out_ref):
    slots = text_ref.shape[0]
    row = lax.broadcasted_iota(jnp.int32, (slots, slots), 0)
    col = lax.broadcasted_iota(jnp.int32, (slots, slots), 1)
    spread = (row == place_ref[...]).astype(F32).astype(BF)
    visual = vis_ref[...] > 0
    placed = jnp.dot(spread, in_ref[...], preferred_element_type=F32)
    qkv = jnp.where(visual, placed, text_ref[...].astype(F32)).astype(BF)
    allowed = (sega_ref[...] == segb_ref[...]) & (col <= row)
    width = out_ref.shape[1]
    keys, values = qkv[:, width : width + LHD], qkv[:, width + LHD :]
    for head in range(width // LHD):
        scores = lax.dot_general(
            qkv[:, head * LHD : (head + 1) * LHD], keys, (((1,), (1,)), ((), ())), preferred_element_type=F32
        ) * (1.0 / math.sqrt(LHD))
        scores = jnp.where(allowed, scores, NEG_FILL)
        highest = jnp.max(scores, axis=-1, keepdims=True)
        weights = jnp.where(allowed, jnp.exp(scores - highest), 0.0)
        totals = jnp.sum(weights, axis=-1, keepdims=True)
        mixed = jnp.dot(weights.astype(BF), values, preferred_element_type=F32)
        out_ref[:, head * LHD : (head + 1) * LHD] = (mixed / totals).astype(BF)


def columns_kernel(pos_ref, source_ref, mine_ref, theirs_ref, sems):
    width = mine_ref.shape[2]
    copies = []
    for d in range(4):
        for i, (ref, core) in enumerate(((mine_ref, pos_ref[3]), (theirs_ref, 1 - pos_ref[3]))):
            start = pl.multiple_of((2 * ((pos_ref[2] + d) % 4) + core) * width, width)
            copies.append(pltpu.make_async_copy(source_ref.at[:, pl.ds(start, width)], ref.at[d], sems.at[d, i]))
    for copy in copies:
        copy.start()
    for copy in copies:
        copy.wait()


def block_kernel(mine_ref, theirs_ref, right_ref, other_ref, *outs):
    both = jnp.dot(theirs_ref[...], other_ref[0], preferred_element_type=F32) + jnp.dot(
        mine_ref[...], right_ref[0], preferred_element_type=F32
    )
    rows = outs[0].shape[0]
    for i, out in enumerate(outs):
        out[...] = both[i * rows : (i + 1) * rows].astype(BF)


def column_block(mine, theirs, right, other, d, count):
    depth, width = right.shape[1:]
    rows = mine.shape[0] // count
    whole = lambda shape: pl.BlockSpec(shape, lambda i: (0, 0))
    block = pl.BlockSpec((1, depth, width), lambda i: (d, 0, 0))
    return pl.pallas_call(
        block_kernel,
        grid=(1,),
        in_specs=[whole(mine.shape), whole(mine.shape), block, block],
        out_specs=[whole((rows, width))] * count,
        out_shape=[jax.ShapeDtypeStruct((rows, width), BF)] * count,
        compiler_params=limit(16),
        name="block_kernel",
    )(mine, theirs, right, other)


def body(
    patches, image_ids, vision_gain, v_query, v_key, v_value, v_out, merge_gain, merge_up, merge_down,
    owners, text_embed, segment_ids, lang_gain, l_query, l_key, l_value, l_out,
):
    x, y, z, c = (lax.axis_index(a) for a in ("x", "y", "z", "c"))
    seq_index = 4 * x + y
    row_count = patches.shape[0]
    tokens = row_count // 4
    local = v_query.shape[1]

    pos = jnp.stack([x, y, z, c]).astype(jnp.int32)
    scalars = pl.BlockSpec(memory_space=pltpu.SMEM)
    vmem = pl.BlockSpec(memory_space=pltpu.VMEM)

    key_value, query_own, *cut = pl.pallas_call(
        project_kernel,
        in_specs=[scalars] + [vmem] * 6,
        out_specs=[vmem] * 10,
        out_shape=[
            jax.ShapeDtypeStruct((2 * local, row_count), BF),
            jax.ShapeDtypeStruct((local, row_count), BF),
        ]
        + [jax.ShapeDtypeStruct((tokens, DV), BF)]
        + [jax.ShapeDtypeStruct((tokens // 2, DV), BF)] * 3
        + [jax.ShapeDtypeStruct((merge_down.shape[0], merge_down.shape[1] // 4), BF)] * 4,
        name="project_kernel",
    )(pos, patches, vision_gain, v_query.T, v_key.T, v_value.T, merge_down)
    picked, quarters = cut[:4], cut[4:]
    seq = ("x", "y")
    left, right = shift(key_value, seq, 1), shift(key_value, seq, -1)
    padded_ids = jnp.pad(image_ids, (tokens, tokens), constant_values=-1)
    near_ids = lax.dynamic_slice_in_dim(padded_ids, seq_index * tokens, 3 * tokens)
    attended = pl.pallas_call(
        vision_kernel,
        in_specs=[scalars] + [vmem] * 5,
        out_specs=[vmem] * 4,
        out_shape=[jax.ShapeDtypeStruct((local, tokens), BF)] * 4,
        scratch_shapes=[
            pltpu.VMEM((2, local, row_count // 2), BF),
            pltpu.VMEM((local, 3 * row_count), BF),
            pltpu.VMEM((local, 3 * row_count), BF),
            pltpu.VMEM((2, local, row_count // 2), BF),
        ],
        compiler_params=limit(24),
        name="vision_kernel",
    )(
        pos, query_own, key_value, left, right, near_ids[None, :]
    )

    token_at = jnp.arange(tokens, dtype=jnp.int32)
    down_z = [quarters[0]] + [shift(quarters[e], "z", e) for e in (1, 2, 3)]
    out_parts = gather_direct(after(v_out, query_own), "z")

    att_moved = [attended[0]] + [shift(attended[d], "x", d) for d in (1, 2, 3)]
    up_parts = gather_halves(after(merge_up, attended[0]), "y")
    att_rows = jnp.concatenate(att_moved, axis=1)
    att_z = gather_direct(att_rows, "z")
    up_parts = far_halves(up_parts, "y", att_rows)
    moved_patches = [shift(after(picked[d], att_rows), "x", d) for d in (1, 2, 3)]
    residual = [picked[0]] + [v for p in moved_patches for v in (p, swap_cores(p))]
    text_parts = gather_halves(after(after(text_embed, att_z[2]), att_z[1]), "z")
    att_all = [v for block in att_z for v in (block, swap_cores(block))]
    out_all = [v for part in out_parts for v in (part, swap_cores(after(part, att_rows)))]
    down_terms = pl.pallas_call(
        regroup_kernel,
        in_specs=[scalars] + [vmem] * 4,
        out_specs=[vmem] * 4,
        out_shape=[jax.ShapeDtypeStruct(quarters[0].shape, BF)] * 4,
        compiler_params=limit(8),
        name="regroup_kernel",
    )(pos, *[after(part, attended[0]) for part in down_z])
    down_own = [down_terms[0]] + [shift(down_terms[e], "x", e) for e in (1, 2, 3)]
    down_parts = gather_halves(jnp.stack([after(part, att_rows) for part in down_own]), "y")
    up_terms = pl.pallas_call(
        merge_kernel,
        in_specs=[scalars] + [vmem] * 29,
        out_specs=[vmem] * 4,
        out_shape=[jax.ShapeDtypeStruct((local, row_count), BF)] * 4,
        scratch_shapes=[
            pltpu.VMEM((8 * local, row_count), BF),
            pltpu.VMEM((8 * local, DV), BF),
            pltpu.VMEM((4 * merge_up.shape[0], merge_up.shape[1]), BF),
            pltpu.VMEM((4 * local, row_count), BF),
            pltpu.VMEM((row_count, DV), BF),
        ],
        compiler_params=limit(32),
        name="merge_kernel",
    )(pos, *att_all, *out_all, *residual, merge_gain, *up_parts)
    hidden_sum = reduce_direct(up_terms, "x")
    hidden = jax.nn.gelu(hidden_sum, approximate=False).astype(BF)
    down_parts = far_halves(down_parts, "y", up_terms[0])
    hidden_z = gather_direct(hidden, "z")
    hidden_all = [v for block in hidden_z for v in (block, swap_cores(block))]
    text_parts = far_halves(text_parts, "z", hidden)
    down_all = down_parts + [swap_cores(part) for part in down_parts]
    down_terms = pl.pallas_call(
        down_kernel,
        in_specs=[scalars] + [vmem] * 18,
        out_specs=[vmem] * 4,
        out_shape=[jax.ShapeDtypeStruct((tokens, 2 * merge_down.shape[1]), BF)] * 4,
        scratch_shapes=[pltpu.VMEM((8 * local, row_count), BF), pltpu.VMEM((8 * local, 2 * merge_down.shape[1]), BF)],
        compiler_params=limit(24),
        name="down_kernel",
    )(pos, *hidden_all, *down_all)
    merged = reduce_direct(down_terms, "x").astype(BF)
    merged_z = gather_direct(merged, "z")
    merged_blocks = [v for block in merged_z for v in (block, swap_cores(block))]
    text_all = text_parts + [swap_cores(after(part, hidden)) for part in text_parts]
    projections = (l_query, l_key, l_value)
    (text_qkv,) = language_rows(pos, text_all, lang_gain, projections)

    owner_count = 16
    pair_cap = 2 * tokens // owner_count
    destination = owners[:, 0]
    owner_iota = jnp.arange(owner_count, dtype=jnp.int32)
    my_destination = lax.dynamic_slice_in_dim(destination, seq_index * tokens, tokens)
    earlier = token_at[None, :] < token_at[:, None]
    local_rank = jnp.sum(((my_destination[:, None] == my_destination[None, :]) & earlier).astype(jnp.int32), axis=1)
    send_index = my_destination * pair_cap + local_rank
    from_each = jnp.sum((destination.reshape(owner_count, tokens) == seq_index).astype(jnp.int32), axis=1)
    lower = owner_iota[None, :] < owner_iota[:, None]
    offsets = jnp.sum(jnp.where(lower, from_each[None, :], 0), axis=1)
    pair_rank = jnp.arange(pair_cap, dtype=jnp.int32)
    slot_count = text_embed.shape[0]
    placement = jnp.where(
        pair_rank[None, :] < from_each[:, None], offsets[:, None] + pair_rank[None, :], slot_count
    ).reshape(-1)
    slot_at = jnp.arange(slot_count, dtype=jnp.int32)
    is_vision = slot_at < jnp.sum(from_each)


    outgoing, own_outgoing = language_rows(pos, merged_blocks, lang_gain, projections, send_index[None, :])
    l_width = text_embed.shape[1]
    own_out, their_out = pl.pallas_call(
        columns_kernel,
        in_specs=[scalars, pl.BlockSpec(memory_space=pltpu.HBM)],
        out_specs=[vmem] * 2,
        out_shape=[jax.ShapeDtypeStruct((4, l_out.shape[0], l_width), BF)] * 2,
        scratch_shapes=[pltpu.SemaphoreType.DMA((4, 2))],
        compiler_params=limit(16),
        name="columns_kernel",
    )(pos, after(l_out, merged))
    other_out = swap_cores(their_out)

    def route(rows):
        arrived = lax.all_to_all(
            rows.reshape(owner_count, pair_cap, -1), seq, split_axis=0, concat_axis=0, tiled=True
        )
        return arrived.reshape(owner_count * pair_cap, -1)

    incoming = route(outgoing)
    own_incoming = route(own_outgoing)
    visual = is_vision.astype(jnp.int32)[:, None]
    lang_attended = pl.pallas_call(
        language_kernel,
        out_shape=jax.ShapeDtypeStruct((slot_count, l_query.shape[1]), BF),
        compiler_params=limit(16),
        name="language_kernel",
    )(incoming, text_qkv, placement[None, :], visual, segment_ids[:, None], segment_ids[None, :])
    filled = pl.pallas_call(
        fill_kernel,
        out_shape=jax.ShapeDtypeStruct(text_embed.shape, BF),
        compiler_params=limit(16),
        name="fill_kernel",
    )(own_incoming, text_embed, placement[None, :], visual)

    theirs = swap_cores(lang_attended)

    def block(d, count):
        return column_block(lang_attended, theirs, own_out, other_out, d, count)

    far = block(2, 2)
    after_one, before_one, own = block(1, 2), block(3, 2), block(0, 1)
    up, down = shift(far[0], "z", 1), shift(far[1], "z", -1)
    nxt_high, prv_low = shift(after_one[1], "z", 1), shift(before_one[0], "z", -1)
    nxt_low = shift((after_one[0].astype(F32) + up.astype(F32)).astype(BF), "z", 1)
    prv_high = shift((before_one[1].astype(F32) + down.astype(F32)).astype(BF), "z", -1)
    total = jnp.concatenate(
        [nxt_low.astype(F32) + prv_low.astype(F32), nxt_high.astype(F32) + prv_high.astype(F32)], axis=0
    )
    return (filled.astype(F32) + own[0].astype(F32) + total).astype(BF)


def solution(mesh):
    fine = Mesh(mesh.devices.reshape(4, 4, 4, 2), ("x", "y", "z", "c"))
    seq, tp = ("x", "y"), ("z", "c")
    in_specs = (
        P(seq, None), P(), P(), P(None, tp), P(None, tp), P(None, tp), P(tp, None), P(), P(seq, tp), P(tp, seq),
        P(), P(seq, tp), P(seq), P(), P(None, tp), P(None, tp), P(None, tp), P(tp, None),
    )


    return jax.shard_map(body, mesh=fine, in_specs=in_specs, out_specs=P(seq, tp), check_vma=False)
```

```python
import math

import jax
import jax.numpy as jnp
from jax import lax
from jax.experimental import pallas as pl
from jax.experimental.pallas import tpu as pltpu
from jax.sharding import Mesh
from jax.sharding import PartitionSpec as P

DV = 1280
VHEADS = 16
D = 8192
LHD = 128
HEAD = DV // VHEADS
EPSILON = 1e-06
NEG_FILL = -1e30
BF = jnp.bfloat16
F32 = jnp.float32


def shift(value, axis, step):
    count = lax.axis_size(axis)
    return lax.ppermute(value, axis, [(i, (i + step) % count) for i in range(count)])


def after(value, other):
    return lax.optimization_barrier((value, other))[0]


def limit(mebibytes):
    return pltpu.CompilerParams(vmem_limit_bytes=mebibytes << 20)


def gather_direct(value, axis):
    return [value] + [shift(value, axis, d) for d in (1, 2, 3)]


def gather_halves(value, axis):
    return [value, shift(value, axis, 1), shift(value, axis, -1)]


def far_halves(parts, axis, held):
    half = parts[0].shape[0] // 2
    before, behind = after(parts[1], held), after(parts[2], held)
    low, high = shift(before[:half], axis, 1), shift(behind[half:], axis, -1)
    return parts + [low, high]


def swap_cores(value):
    return shift(value, "c", 1)


def reduce_direct(blocks, axis):
    total = blocks[0].astype(F32)
    for d in (1, 2, 3):
        total = total + shift(blocks[d], axis, d).astype(F32)
    return total


def rms_scaled(values, norm_gain):
    mean_square = jnp.mean(values * values, axis=-1, keepdims=True)
    return (values * lax.rsqrt(mean_square + EPSILON) * norm_gain).astype(BF)


def project_kernel(pos_ref, x_ref, gain_ref, wq_ref, wk_ref, wv_ref, down_ref, kv_ref, q_ref, *rest):
    normed = rms_scaled(x_ref[...].astype(F32), gain_ref[...][None, :])
    width = wq_ref.shape[0]

    def project(weight):
        return lax.dot_general(weight, normed, (((1,), (1,)), ((), ())), preferred_element_type=F32).astype(BF)

    kv_ref[:width] = project(wk_ref[...])
    kv_ref[width:] = project(wv_ref[...])
    q_ref[...] = project(wq_ref[...])
    picked, quarters = rest[:4], rest[4:]
    narrow = quarters[0].shape[1]
    for e in range(4):
        start = pl.multiple_of((pos_ref[2] + e) % 4 * narrow, narrow)
        quarters[e][...] = down_ref[:, pl.ds(start, narrow)]
    count = x_ref.shape[0]
    for d in range(4):
        tokens = picked[d].shape[0]
        token = lax.broadcasted_iota(jnp.int32, (tokens, count), 0) + (pos_ref[3] * tokens if d else 0)
        patch = lax.broadcasted_iota(jnp.int32, (tokens, count), 1)
        pick = (patch == 4 * token + (pos_ref[0] + d) % 4).astype(F32).astype(BF)
        picked[d][...] = jnp.dot(pick, x_ref[...], preferred_element_type=F32).astype(BF)


def vision_kernel(pos_ref, q_ref, own_ref, left_ref, right_ref, id_ref, *refs):
    outs, (queries_s, keys_s, values_s, mixed_s) = refs[:4], refs[4:]
    rows, count = q_ref.shape
    tokens, wide = count // 4, count // 2
    column = lax.broadcasted_iota(jnp.int32, (count, count), 1)
    source = lax.broadcasted_iota(jnp.int32, (count, count), 0)
    wanted = 4 * (column % tokens) + (column // tokens + pos_ref[0]) % 4
    order = (source == wanted).astype(F32).astype(BF)
    queries = jnp.dot(q_ref[...], order, preferred_element_type=F32).astype(BF)
    for part in range(2):
        queries_s[part] = queries[:, part * wide : (part + 1) * wide]
    for i, ref in enumerate((own_ref, left_ref, right_ref)):
        keys_s[:, i * count : (i + 1) * count] = ref[:rows]
        values_s[:, i * count : (i + 1) * count] = ref[rows:]
    patch = lax.broadcasted_iota(jnp.int32, (count, tokens), 0)
    token = lax.broadcasted_iota(jnp.int32, (count, tokens), 1)
    owner = (patch // 4 == token).astype(F32).astype(BF)
    ids = id_ref[...].astype(F32)
    key_ids = [
        lax.dot_general(
            owner, jnp.broadcast_to(ids[:, i * tokens : (i + 1) * tokens], (8, tokens)).astype(BF),
            (((1,), (1,)), ((), ())), preferred_element_type=F32,
        )[:, :1]
        for i in (1, 0, 2)
    ]
    own_ids = ids[:, tokens : 2 * tokens]
    allowed = jnp.concatenate(key_ids, axis=0) == jnp.concatenate([own_ids, own_ids], axis=1)
    scale = math.log2(math.e) / math.sqrt(HEAD)

    def one(step, _):
        lower = pl.multiple_of(step // 2 * HEAD, HEAD)
        scores = lax.dot_general(
            keys_s[pl.ds(lower, HEAD)], queries_s[step % 2, pl.ds(lower, HEAD)],
            (((0,), (0,)), ((), ())), preferred_element_type=F32,
        )
        scores = jnp.where(allowed, scores * scale, NEG_FILL)
        highest = jnp.max(scores, axis=0, keepdims=True)
        weights = jnp.exp2(scores - highest)
        totals = jnp.sum(weights, axis=0, keepdims=True)
        mixed = jnp.dot(values_s[pl.ds(lower, HEAD)], weights.astype(BF), preferred_element_type=F32)
        mixed_s[step % 2, pl.ds(lower, HEAD)] = (mixed / totals).astype(BF)
        return 0

    lax.fori_loop(0, 2 * (rows // HEAD), one, 0)
    for i in range(4):
        outs[i][...] = mixed_s[i // 2, :, i % 2 * tokens : (i % 2 + 1) * tokens]


def merge_kernel(pos_ref, *refs):
    att, weights, rest, (gain_ref, *ups), outs, (att_s, w_s, up_s, t_s, rest_s) = (
        refs[:8], refs[8:16], refs[16:23], refs[23:28], refs[28:32], refs[32:]
    )
    part, tokens = att[0].shape[0], rest[0].shape[0]
    half = tokens // 2
    for i in range(8):
        att_s[i * part : (i + 1) * part] = att[i][...]
    for r in range(4):
        for other in range(2):
            start = (2 * r + other) * part
            w_s[start : start + part] = weights[2 * r + other][...]
    rows = ups[0].shape[0]
    for d, ref in enumerate(ups):
        start = pl.multiple_of((pos_ref[1] + 4 - d) % 4 * rows, rows)
        up_s[pl.ds(start, ref.shape[0])] = ref[...]
    rest_s[:tokens] = rest[0][...]
    for d in range(1, 4):
        for other in range(2):
            start = pl.multiple_of(d * tokens + (pos_ref[3] + other) % 2 * half, half)
            rest_s[pl.ds(start, half)] = rest[2 * d - 1 + other][...]
    state = lax.dot_general(att_s[...], w_s[...], (((0,), (0,)), ((), ())), preferred_element_type=F32)
    state = state + rest_s[...].astype(F32)
    normed = rms_scaled(state, gain_ref[...][None, :])
    t_s[...] = jnp.dot(normed, up_s[...], preferred_element_type=F32).T.astype(BF)
    for e in range(4):
        start = pl.multiple_of((pos_ref[0] + e) % 4 * part, part)
        term = t_s[pl.ds(start, part)]
        for d in range(4):
            g = (d + e) % 4
            outs[e][:, g * tokens : (g + 1) * tokens] = term[:, d * tokens : (d + 1) * tokens]


def regroup_kernel(pos_ref, *refs):
    blocks, outs = refs[:4], refs[4:]
    part = blocks[0].shape[0] // 4
    for e in range(4):
        start = pl.multiple_of((pos_ref[0] + e) % 4 * part, part)
        for r in range(4):
            outs[e][r * part : (r + 1) * part] = blocks[r][pl.ds(start, part)]


def down_kernel(pos_ref, *refs):
    hidden, parts, outs, (h_s, w_s) = refs[:8], refs[8:18], refs[18:22], refs[22:]
    x, y, c = pos_ref[0], pos_ref[1], pos_ref[3]
    part, tokens = hidden[0].shape[0], outs[0].shape[0]
    narrow = parts[0].shape[2]
    for i in range(8):
        h_s[i * part : (i + 1) * part] = hidden[i][...]

    def place(ref, other, d, first):
        for q in range(ref.shape[0]):
            at = (x + 4 - first - q) % 4 * 2 + (y + 4 - d) % 4 // 2
            column = pl.ds(pl.multiple_of(at * narrow, narrow), narrow)
            for r in range(4):
                start = (2 * r + other) * part
                w_s[start : start + part, column] = ref[q, r * part : (r + 1) * part]

    @pl.when((y + c) % 2 == 0)
    def _():
        for other in range(2):
            place(parts[5 * other], other, 0, 0)
            place(parts[5 * other + 3], other, 2, 0)
            place(parts[5 * other + 4], other, 2, 2)

    @pl.when((y + c) % 2 == 1)
    def _():
        for other in range(2):
            place(parts[5 * other + 1], other, 1, 0)
            place(parts[5 * other + 2], other, 3, 0)

    both = lax.dot_general(h_s[...], w_s[...], (((0,), (0,)), ((), ())), preferred_element_type=F32).astype(BF)
    for g in range(4):
        outs[(4 - g) % 4][...] = both[g * tokens : (g + 1) * tokens]


def rows_kernel(pos_ref, *refs, routed):
    count = 8 if routed else 10
    blocks, (gain_ref, *weights), rest = refs[:count], refs[count : count + 4], refs[count + 4 :]
    (send_ref, out_ref, own_ref, s, *buffers, sems) = rest if routed else (None, rest[0], None, rest[1], None)
    rows, width = s.shape[0], s.shape[1] // 8
    z, c = pos_ref[2], pos_ref[3]

    def copies(i):
        return [
            pltpu.make_async_copy(w.at[pl.ds(i * width, width)], b.at[pl.ds(i * width, width)], sems.at[i, j])
            for j, (w, b) in enumerate(zip(weights, buffers))
        ]

    copies_of = [copies(i) for i in range(8)] if routed else []
    for group in copies_of:
        for copy in group:
            copy.start()
    total = jnp.zeros((rows, 1), F32)
    if routed:
        narrow = width // 8
        for i in range(8):
            value = blocks[i][...].astype(F32)
            total = total + jnp.sum(value * value, axis=-1, keepdims=True)
            core = (c + i % 2) % 2
            for k in range(8):
                start = pl.multiple_of((core + 2 * k) * 4 * narrow + (z + 4 - i // 2) % 4 * narrow, narrow)
                s[:, pl.ds(start, narrow)] = blocks[i][:, k * narrow : (k + 1) * narrow]
    else:
        half = rows // 2
        for other in range(2):
            own, before, behind, low, high = blocks[5 * other : 5 * other + 5]
            for r, first, ref in ((0, 0, own), (1, 0, before), (3, 0, behind), (2, 0, low), (2, half, high)):
                start = pl.multiple_of((2 * ((z + 4 - r) % 4) + (c + other) % 2) * width, width)
                s[first : first + ref.shape[0], pl.ds(start, width)] = ref[...]
        for i in range(8):
            value = s[:, i * width : (i + 1) * width].astype(F32)
            total = total + jnp.sum(value * value, axis=-1, keepdims=True)
    scale = lax.rsqrt(total / D + EPSILON)

    def one(i, sums):
        start = i * width if isinstance(i, int) else pl.multiple_of(i * width, width)
        columns = pl.ds(start, width)
        normed = (s[:, columns].astype(F32) * scale * gain_ref[:, columns]).astype(BF)
        return tuple(t + jnp.dot(normed, w[columns], preferred_element_type=F32) for t, w in zip(sums, weights))

    sums = tuple(jnp.zeros((rows, w.shape[1]), F32) for w in weights)
    if routed:
        weights = buffers
        for i in range(8):
            for copy in copies_of[i]:
                copy.wait()
            sums = one(i, sums)
    else:
        sums = lax.fori_loop(0, 8, one, sums)
    whole = jnp.concatenate(sums, axis=1).astype(BF)
    if routed:
        pick = (lax.broadcasted_iota(jnp.int32, (out_ref.shape[0], rows), 0) == send_ref[...]).astype(F32).astype(BF)
        out_ref[...] = jnp.dot(pick, whole, preferred_element_type=F32).astype(BF)
        own = s[:, pl.ds(pl.multiple_of((2 * z + c) * width, width), width)]
        own_ref[...] = jnp.dot(pick, own, preferred_element_type=F32).astype(BF)
    else:
        out_ref[...] = whole


def language_rows(pos, blocks, gain, weights, send=None):
    rows, width = blocks[0].shape
    total = sum(w.shape[1] for w in weights)
    operands = [pos, *blocks, gain[None, :], *weights]
    vmem = pl.BlockSpec(memory_space=pltpu.VMEM)
    where = vmem if send is None else pl.BlockSpec(memory_space=pltpu.HBM)
    specs = [pl.BlockSpec(memory_space=pltpu.SMEM)] + [vmem] * (len(blocks) + 1) + [where] * 3
    scratch = [pltpu.VMEM((rows, 8 * width), BF)]
    shapes = [jax.ShapeDtypeStruct((rows, total), BF)]
    if send is not None:
        operands.append(send)
        specs.append(vmem)
        scratch += [pltpu.VMEM(w.shape, BF) for w in weights] + [pltpu.SemaphoreType.DMA((8, 3))]
        shapes = [jax.ShapeDtypeStruct((2 * rows, n), BF) for n in (total, width)]
    return pl.pallas_call(
        lambda *refs: rows_kernel(*refs, routed=send is not None),
        in_specs=specs,
        out_specs=[vmem] * len(shapes),
        out_shape=shapes,
        scratch_shapes=scratch,
        compiler_params=limit(32 if send is None else 60),
        name="rows_kernel",
    )(*operands)


def fill_kernel(in_ref, embed_ref, place_ref, vis_ref, out_ref):
    slots = embed_ref.shape[0]
    spread = (lax.broadcasted_iota(jnp.int32, (slots, slots), 0) == place_ref[...]).astype(F32).astype(BF)
    placed = jnp.dot(spread, in_ref[...], preferred_element_type=F32)
    out_ref[...] = jnp.where(vis_ref[...] > 0, placed, embed_ref[...].astype(F32)).astype(BF)


def language_kernel(in_ref, text_ref, place_ref, vis_ref, sega_ref, segb_ref, out_ref):
    slots = text_ref.shape[0]
    row = lax.broadcasted_iota(jnp.int32, (slots, slots), 0)
    col = lax.broadcasted_iota(jnp.int32, (slots, slots), 1)
    spread = (row == place_ref[...]).astype(F32).astype(BF)
    visual = vis_ref[...] > 0
    placed = jnp.dot(spread, in_ref[...], preferred_element_type=F32)
    qkv = jnp.where(visual, placed, text_ref[...].astype(F32)).astype(BF)
    allowed = (sega_ref[...] == segb_ref[...]) & (col <= row)
    width = out_ref.shape[1]
    keys, values = qkv[:, width : width + LHD], qkv[:, width + LHD :]
    for head in range(width // LHD):
        scores = lax.dot_general(
            qkv[:, head * LHD : (head + 1) * LHD], keys, (((1,), (1,)), ((), ())), preferred_element_type=F32
        ) * (math.log2(math.e) / math.sqrt(LHD))
        scores = jnp.where(allowed, scores, NEG_FILL)
        highest = jnp.max(scores, axis=-1, keepdims=True)
        weights = jnp.exp2(scores - highest)
        totals = jnp.sum(weights, axis=-1, keepdims=True)
        mixed = jnp.dot(weights.astype(BF), values, preferred_element_type=F32)
        out_ref[:, head * LHD : (head + 1) * LHD] = (mixed / totals).astype(BF)


def columns_kernel(pos_ref, source_ref, mine_ref, theirs_ref, sems):
    width = mine_ref.shape[2]
    copies = []
    for d in range(4):
        for i, (ref, core) in enumerate(((mine_ref, pos_ref[3]), (theirs_ref, 1 - pos_ref[3]))):
            start = pl.multiple_of((2 * ((pos_ref[2] + d) % 4) + core) * width, width)
            copies.append(pltpu.make_async_copy(source_ref.at[:, pl.ds(start, width)], ref.at[d], sems.at[d, i]))
    for copy in copies:
        copy.start()
    for copy in copies:
        copy.wait()


def block_kernel(mine_ref, theirs_ref, right_ref, other_ref, *outs):
    both = jnp.dot(theirs_ref[...], other_ref[0], preferred_element_type=F32) + jnp.dot(
        mine_ref[...], right_ref[0], preferred_element_type=F32
    )
    rows = outs[0].shape[0]
    for i, out in enumerate(outs):
        out[...] = both[i * rows : (i + 1) * rows].astype(BF)


def column_block(mine, theirs, right, other, d, count):
    depth, width = right.shape[1:]
    rows = mine.shape[0] // count
    whole = lambda shape: pl.BlockSpec(shape, lambda i: (0, 0))
    block = pl.BlockSpec((1, depth, width), lambda i: (d, 0, 0))
    return pl.pallas_call(
        block_kernel,
        grid=(1,),
        in_specs=[whole(mine.shape), whole(mine.shape), block, block],
        out_specs=[whole((rows, width))] * count,
        out_shape=[jax.ShapeDtypeStruct((rows, width), BF)] * count,
        compiler_params=limit(16),
        name="block_kernel",
    )(mine, theirs, right, other)


def body(
    patches, image_ids, vision_gain, v_query, v_key, v_value, v_out, merge_gain, merge_up, merge_down,
    owners, text_embed, segment_ids, lang_gain, l_query, l_key, l_value, l_out,
):
    x, y, z, c = (lax.axis_index(a) for a in ("x", "y", "z", "c"))
    seq_index = 4 * x + y
    row_count = patches.shape[0]
    tokens = row_count // 4
    local = v_query.shape[1]

    pos = jnp.stack([x, y, z, c]).astype(jnp.int32)
    scalars = pl.BlockSpec(memory_space=pltpu.SMEM)
    vmem = pl.BlockSpec(memory_space=pltpu.VMEM)

    key_value, query_own, *cut = pl.pallas_call(
        project_kernel,
        in_specs=[scalars] + [vmem] * 6,
        out_specs=[vmem] * 10,
        out_shape=[
            jax.ShapeDtypeStruct((2 * local, row_count), BF),
            jax.ShapeDtypeStruct((local, row_count), BF),
        ]
        + [jax.ShapeDtypeStruct((tokens, DV), BF)]
        + [jax.ShapeDtypeStruct((tokens // 2, DV), BF)] * 3
        + [jax.ShapeDtypeStruct((merge_down.shape[0], merge_down.shape[1] // 4), BF)] * 4,
        name="project_kernel",
    )(pos, patches, vision_gain, v_query.T, v_key.T, v_value.T, merge_down)
    picked, quarters = cut[:4], cut[4:]
    seq = ("x", "y")
    left, right = shift(key_value, seq, 1), shift(key_value, seq, -1)
    padded_ids = jnp.pad(image_ids, (tokens, tokens), constant_values=-1)
    near_ids = lax.dynamic_slice_in_dim(padded_ids, seq_index * tokens, 3 * tokens)
    attended = pl.pallas_call(
        vision_kernel,
        in_specs=[scalars] + [vmem] * 5,
        out_specs=[vmem] * 4,
        out_shape=[jax.ShapeDtypeStruct((local, tokens), BF)] * 4,
        scratch_shapes=[
            pltpu.VMEM((2, local, row_count // 2), BF),
            pltpu.VMEM((local, 3 * row_count), BF),
            pltpu.VMEM((local, 3 * row_count), BF),
            pltpu.VMEM((2, local, row_count // 2), BF),
        ],
        compiler_params=limit(24),
        name="vision_kernel",
    )(
        pos, query_own, key_value, left, right, near_ids[None, :]
    )

    token_at = jnp.arange(tokens, dtype=jnp.int32)
    down_z = [quarters[0]] + [shift(quarters[e], "z", e) for e in (1, 2, 3)]
    out_parts = gather_direct(after(v_out, query_own), "z")

    att_moved = [attended[0]] + [shift(attended[d], "x", d) for d in (1, 2, 3)]
    up_parts = gather_direct(after(merge_up, attended[0]), "y")
    att_rows = jnp.concatenate(att_moved, axis=1)
    att_z = gather_direct(att_rows, "z")
    moved_patches = [shift(after(picked[d], att_rows), "x", d) for d in (1, 2, 3)]
    residual = [picked[0]] + [v for p in moved_patches for v in (p, swap_cores(p))]
    text_parts = gather_halves(after(text_embed, att_rows), "z")
    att_all = [v for block in att_z for v in (block, swap_cores(block))]
    out_all = [v for part in out_parts for v in (part, swap_cores(after(part, att_rows)))]
    down_terms = pl.pallas_call(
        regroup_kernel,
        in_specs=[scalars] + [vmem] * 4,
        out_specs=[vmem] * 4,
        out_shape=[jax.ShapeDtypeStruct(quarters[0].shape, BF)] * 4,
        compiler_params=limit(8),
        name="regroup_kernel",
    )(pos, *[after(part, attended[0]) for part in down_z])
    down_own = [down_terms[0]] + [shift(down_terms[e], "x", e) for e in (1, 2, 3)]
    down_parts = gather_halves(jnp.stack([after(part, att_rows) for part in down_own]), "y")
    up_terms = pl.pallas_call(
        merge_kernel,
        in_specs=[scalars] + [vmem] * 28,
        out_specs=[vmem] * 4,
        out_shape=[jax.ShapeDtypeStruct((local, row_count), BF)] * 4,
        scratch_shapes=[
            pltpu.VMEM((8 * local, row_count), BF),
            pltpu.VMEM((8 * local, DV), BF),
            pltpu.VMEM((4 * merge_up.shape[0], merge_up.shape[1]), BF),
            pltpu.VMEM((4 * local, row_count), BF),
            pltpu.VMEM((row_count, DV), BF),
        ],
        compiler_params=limit(32),
        name="merge_kernel",
    )(pos, *att_all, *out_all, *residual, merge_gain, *up_parts)
    hidden_sum = reduce_direct(up_terms, "x")
    hidden = jax.nn.gelu(hidden_sum, approximate=False).astype(BF)
    down_parts = far_halves(down_parts, "y", up_terms[0])
    hidden_z = gather_direct(hidden, "z")
    hidden_all = [v for block in hidden_z for v in (block, swap_cores(block))]
    text_parts = far_halves(text_parts, "z", hidden)
    down_all = down_parts + [swap_cores(part) for part in down_parts]
    down_terms = pl.pallas_call(
        down_kernel,
        in_specs=[scalars] + [vmem] * 18,
        out_specs=[vmem] * 4,
        out_shape=[jax.ShapeDtypeStruct((tokens, 2 * merge_down.shape[1]), BF)] * 4,
        scratch_shapes=[pltpu.VMEM((8 * local, row_count), BF), pltpu.VMEM((8 * local, 2 * merge_down.shape[1]), BF)],
        compiler_params=limit(24),
        name="down_kernel",
    )(pos, *hidden_all, *down_all)
    merged = reduce_direct(down_terms, "x").astype(BF)
    merged_z = gather_direct(merged, "z")
    merged_blocks = [v for block in merged_z for v in (block, swap_cores(block))]
    text_all = text_parts + [swap_cores(after(part, hidden)) for part in text_parts]
    projections = (l_query, l_key, l_value)
    (text_qkv,) = language_rows(pos, text_all, lang_gain, projections)

    owner_count = 16
    pair_cap = 2 * tokens // owner_count
    destination = owners[:, 0]
    owner_iota = jnp.arange(owner_count, dtype=jnp.int32)
    my_destination = lax.dynamic_slice_in_dim(destination, seq_index * tokens, tokens)
    earlier = token_at[None, :] < token_at[:, None]
    local_rank = jnp.sum(((my_destination[:, None] == my_destination[None, :]) & earlier).astype(jnp.int32), axis=1)
    send_index = my_destination * pair_cap + local_rank
    from_each = jnp.sum((destination.reshape(owner_count, tokens) == seq_index).astype(jnp.int32), axis=1)
    lower = owner_iota[None, :] < owner_iota[:, None]
    offsets = jnp.sum(jnp.where(lower, from_each[None, :], 0), axis=1)
    pair_rank = jnp.arange(pair_cap, dtype=jnp.int32)
    slot_count = text_embed.shape[0]
    placement = jnp.where(
        pair_rank[None, :] < from_each[:, None], offsets[:, None] + pair_rank[None, :], slot_count
    ).reshape(-1)
    slot_at = jnp.arange(slot_count, dtype=jnp.int32)
    is_vision = slot_at < jnp.sum(from_each)


    outgoing, own_outgoing = language_rows(pos, merged_blocks, lang_gain, projections, send_index[None, :])
    l_width = text_embed.shape[1]
    own_out, their_out = pl.pallas_call(
        columns_kernel,
        in_specs=[scalars, pl.BlockSpec(memory_space=pltpu.HBM)],
        out_specs=[vmem] * 2,
        out_shape=[jax.ShapeDtypeStruct((4, l_out.shape[0], l_width), BF)] * 2,
        scratch_shapes=[pltpu.SemaphoreType.DMA((4, 2))],
        compiler_params=limit(16),
        name="columns_kernel",
    )(pos, after(l_out, merged))
    other_out = swap_cores(their_out)

    def route(rows):
        arrived = lax.all_to_all(
            rows.reshape(owner_count, pair_cap, -1), seq, split_axis=0, concat_axis=0, tiled=True
        )
        return arrived.reshape(owner_count * pair_cap, -1)

    incoming = route(outgoing)
    own_incoming = route(own_outgoing)
    visual = is_vision.astype(jnp.int32)[:, None]
    lang_attended = pl.pallas_call(
        language_kernel,
        out_shape=jax.ShapeDtypeStruct((slot_count, l_query.shape[1]), BF),
        compiler_params=limit(16),
        name="language_kernel",
    )(incoming, text_qkv, placement[None, :], visual, segment_ids[:, None], segment_ids[None, :])
    filled = pl.pallas_call(
        fill_kernel,
        out_shape=jax.ShapeDtypeStruct(text_embed.shape, BF),
        compiler_params=limit(16),
        name="fill_kernel",
    )(own_incoming, text_embed, placement[None, :], visual)

    theirs = swap_cores(lang_attended)

    def block(d, count):
        return column_block(lang_attended, theirs, own_out, other_out, d, count)

    far = block(2, 2)
    after_one, before_one, own = block(1, 2), block(3, 2), block(0, 1)
    up, down = shift(far[0], "z", 1), shift(far[1], "z", -1)
    nxt_high, prv_low = shift(after_one[1], "z", 1), shift(before_one[0], "z", -1)
    nxt_low = shift((after_one[0].astype(F32) + up.astype(F32)).astype(BF), "z", 1)
    prv_high = shift((before_one[1].astype(F32) + down.astype(F32)).astype(BF), "z", -1)
    total = jnp.concatenate(
        [nxt_low.astype(F32) + prv_low.astype(F32), nxt_high.astype(F32) + prv_high.astype(F32)], axis=0
    )
    return (filled.astype(F32) + own[0].astype(F32) + total).astype(BF)


def solution(mesh):
    fine = Mesh(mesh.devices.reshape(4, 4, 4, 2), ("x", "y", "z", "c"))
    seq, tp = ("x", "y"), ("z", "c")
    in_specs = (
        P(seq, None), P(), P(), P(None, tp), P(None, tp), P(None, tp), P(tp, None), P(), P(seq, tp), P(tp, seq),
        P(), P(seq, tp), P(seq), P(), P(None, tp), P(None, tp), P(None, tp), P(tp, None),
    )


    return jax.shard_map(body, mesh=fine, in_specs=in_specs, out_specs=P(seq, tp), check_vma=False)
```
